512 devices in a mesh: groups: 2 (over y), seq: 32 (over z), batch: 4 (over x), head: 2 (over core).
Axes of the slice: x: 4, y: 2, z: 32, core: 2. Of those that a mesh axis runs over, the one named last changes fastest.
The devices are a block of a 4x8x32 slice.
Arguments:
- query_in: bfloat16 [8, 16384, 1024], P(('groups', 'batch'), 'seq', 'head'), parts along dimension 0, may hold values from -1.5 to 1.5
- key_in: bfloat16 [8, 16384, 1024], P(('groups', 'batch'), 'seq', 'head'), parts along dimension 0, may hold values from -1.5 to 1.5
- value_in: bfloat16 [8, 16384, 1024], P(('groups', 'batch'), 'seq', 'head'), parts along dimension 0, may hold values from -6 to 6
- level_mask: int32 [8, 16384, 16], P(('groups', 'batch'), 'seq'), parts along dimension 0, may hold values 0 or 1
- out_weight: bfloat16 [1024, 2048], P('head'), may hold values from -0.1875 to 0.1875
- grad_out: bfloat16 [8, 16384, 2048], P(('groups', 'batch'), 'seq', 'head'), parts along dimension 0, may hold values from -0.8984375 to 0.8984375
Outputs:
- layer_out: bfloat16 [8, 16384, 2048], P(('groups', 'batch'), 'seq', 'head'), parts along dimension 0
- grad_query: bfloat16 [8, 16384, 1024], P(('groups', 'batch'), 'seq', 'head'), parts along dimension 0
- grad_key: bfloat16 [8, 16384, 1024], P(('groups', 'batch'), 'seq', 'head'), parts along dimension 0
- grad_value: bfloat16 [8, 16384, 1024], P(('groups', 'batch'), 'seq', 'head'), parts along dimension 0
The draws below stay inside these ranges and needn't reach their ends.
There are 2 independent parts, one for each index of `groups`. The reference program is written for one: setup_inputs(seed, part) draws one part's arguments, and reference() takes and returns one part's arrays. A program takes and returns all parts, laid end to end along the dimension named above; an argument that names none is the same for every part. Nothing has to cross between parts.
All inputs are finite; a program needn't handle non-finite values. No bound on the sum of `level_mask` on one device may be relied on, other than what follows from the above.
Results may differ from the reference program's by a relative error of at most 0.0091.
Values may be sent and summed in bfloat16 or wider, within the bound.
A program may use at most 64 MiB of HBM per device.

```python
import jax
import jax.numpy as jnp
import numpy as np
from jax import lax

D = 2048
H = 8
HEAD_DIM = 128
LEVEL_SLOTS = 16
TOK_DEV = 512
BATCH = 4
TOKENS = 16384
N_SEQ = 32


def with_ends(values, stream_key, low, largest):
    spot = [jax.random.randint(jax.random.fold_in(stream_key, axis), (), 0, length) for axis, length in enumerate(values.shape)]
    main_axis = values.shape.index(max(values.shape))
    neighbour = spot[:main_axis] + [(spot[main_axis] + 1) % values.shape[main_axis]] + spot[main_axis + 1:]
    return values.at[tuple(spot)].set(low).at[tuple(neighbour)].set(largest)


def shard_levels(own_key, shape, cuts, low, top_value):
    level, own = 1.0, jax.random.fold_in(own_key, 6)
    for axis_at, blocks in cuts:
        draws = jnp.exp(jax.random.uniform(jax.random.fold_in(own, axis_at), (blocks,), jnp.float32, low / len(cuts), top_value / len(cuts)))
        level = level * jnp.repeat(draws, shape[axis_at] // blocks).reshape([-1 if axis == axis_at else 1 for axis in range(len(shape))])
    return level


def noise(own_key, shape, width, most, cuts=(), kind=jnp.bfloat16):
    values = width * jax.random.normal(own_key, shape, jnp.float32)
    if cuts:
        values = values * shard_levels(own_key, shape, cuts, -0.22, 0.18)
    return jnp.clip(values, -most, most).astype(kind)


def setup_inputs(seed: int = 0, part: int = 0) -> dict:
    key_of = jax.random.split(jax.random.key(seed), 7)
    part_splits = jax.random.split(jax.random.fold_in(key_of[6], part), 7)
    return {
        "query_in": noise(part_splits[0], (BATCH, TOKENS, H * HEAD_DIM), 0.25, 1.5, ((0, 4), (1, 32), (2, 2))),
        "key_in": noise(part_splits[1], (BATCH, TOKENS, H * HEAD_DIM), 0.25, 1.5, ((0, 4), (1, 32), (2, 2))),
        "value_in": noise(part_splits[2], (BATCH, TOKENS, H * HEAD_DIM), 1.0, 6.0, ((0, 4), (1, 32), (2, 2))),
        "level_mask": with_ends((jax.random.randint(part_splits[3], (BATCH, TOKENS, LEVEL_SLOTS), 0, 4) < 3).astype(jnp.int32), jax.random.fold_in(part_splits[3], 1), 0, 1),
        "out_weight": noise(key_of[4], (H * HEAD_DIM, D), (H * HEAD_DIM) ** -0.5, 0.1875, ((0, 2),)),
        "grad_out": noise(part_splits[5], (BATCH, TOKENS, D), 0.15, 0.8984375, ((0, 4), (1, 32), (2, 2))),
    }


level_scale = np.array([1.0] + [2.0 ** (-(tier - 1) / 2.0) for tier in range(1, 16)], dtype=np.float32)
HIGHEST = lax.Precision.HIGHEST


def top_bit(values):
    result = jnp.zeros_like(values)
    for power in range(1, 24):
        result = result + (values >= (1 << power)).astype(jnp.int32)
    return result


def block_levels(count):
    rows = jnp.arange(count, dtype=jnp.int32)
    later = rows[:, None]
    earlier = rows[None, :]
    spread = jnp.bitwise_xor(later, earlier)
    depth_map = jnp.where(spread == 0, 0, 1 + top_bit(jnp.maximum(spread, 1)))
    inside = earlier <= later
    return jnp.stack([((depth_map == tier) & inside).astype(jnp.float32) for tier in range(count.bit_length())])


def block_routes(count, span):
    rows = jnp.arange(count, dtype=jnp.int32)
    later = rows[:, None]
    earlier = rows[None, :]
    tier_of = top_bit(jnp.maximum(jnp.bitwise_xor(later, earlier), 1))
    return jnp.stack([((earlier < later) & (tier_of == tier)).astype(jnp.float32) for tier in range(span)])


def to_low(values):
    return lax.optimization_barrier(values.astype(jnp.bfloat16)).astype(jnp.float32)


def one_sequence(inputs, out_weight):
    query_seq, key_seq, value_seq, mask_seq, grad_seq = inputs
    shape_blocks = (N_SEQ, TOK_DEV, H, HEAD_DIM)
    query_rows = query_seq.reshape(shape_blocks).astype(jnp.float32)
    key_rows = key_seq.reshape(shape_blocks).astype(jnp.float32)
    value_rows = value_seq.reshape(shape_blocks).astype(jnp.float32)
    weights = mask_seq.astype(jnp.float32).reshape(N_SEQ, TOK_DEV, LEVEL_SLOTS) * jnp.asarray(level_scale, dtype=jnp.float32)
    tiers = TOK_DEV.bit_length()
    span = N_SEQ.bit_length() - 1
    intra_map = block_levels(TOK_DEV)
    blend = jnp.einsum('lts,ntl->nts', intra_map, weights[:, :, :tiers], precision=HIGHEST)
    scores = jnp.einsum('nthd,nshd->nhts', query_rows, key_rows, precision=HIGHEST)
    probs = (scores * blend[:, None]).astype(jnp.bfloat16).astype(jnp.float32)
    local_out = jnp.einsum('nhts,nshd->nthd', probs, value_rows, precision=HIGHEST)
    block_state = jnp.einsum('nthd,nthe->nhde', key_rows, value_rows, precision=HIGHEST)
    routes = block_routes(N_SEQ, span)
    states = jnp.einsum('jbc,chde->jbhde', routes, block_state, precision=HIGHEST)
    states_low = to_low(states)
    tier_weight = weights[:, :, tiers:tiers + span]
    weighted_query = to_low(jnp.transpose(tier_weight, (2, 0, 1))[:, :, :, None, None] * query_rows[None])
    far_out = jnp.einsum('jnthd,jnhde->nthe', weighted_query, states_low, precision=HIGHEST)
    mixed = (local_out + far_out).astype(jnp.bfloat16).reshape(TOKENS, H * HEAD_DIM)
    layer = jnp.dot(mixed, out_weight, preferred_element_type=jnp.float32).astype(jnp.bfloat16)
    grad_mixed = jnp.dot(grad_seq, out_weight.T, preferred_element_type=jnp.float32).astype(jnp.bfloat16)
    grad_rows = grad_mixed.reshape(shape_blocks).astype(jnp.float32)
    dprob = jnp.einsum('nthe,nshe->nhts', grad_rows, value_rows, precision=HIGHEST)
    dscore = (dprob * blend[:, None]).astype(jnp.bfloat16).astype(jnp.float32)
    query_local = jnp.einsum('nhts,nshd->nthd', dscore, key_rows, precision=HIGHEST)
    key_local = jnp.einsum('nhts,nthd->nshd', dscore, query_rows, precision=HIGHEST)
    value_local = jnp.einsum('nhts,nthe->nshe', probs, grad_rows, precision=HIGHEST)
    query_far = jnp.einsum('ntj,nthe,jnhde->nthd', tier_weight, grad_rows, states_low, precision=HIGHEST)
    reach = jnp.einsum('jnthd,nthe->jnhde', weighted_query, grad_rows, precision=HIGHEST)
    back = jnp.einsum('jbc,jbhde->chde', routes, reach, precision=HIGHEST)
    back_low = to_low(back)
    key_far = jnp.einsum('chde,cshe->cshd', back_low, value_rows, precision=HIGHEST)
    value_far = jnp.einsum('chde,cshd->cshe', back_low, key_rows, precision=HIGHEST)
    flat = (TOKENS, H * HEAD_DIM)
    grad_query = (query_local + query_far).astype(jnp.bfloat16).reshape(flat)
    grad_key = (key_local + key_far).astype(jnp.bfloat16).reshape(flat)
    grad_value = (value_local + value_far).astype(jnp.bfloat16).reshape(flat)
    return layer, grad_query, grad_key, grad_value


def reference(query_in, key_in, value_in, level_mask, out_weight, grad_out):
    def apply_one(inputs):
        return one_sequence(inputs, out_weight)
    layer_out, grad_query, grad_key, grad_value = lax.map(apply_one, (query_in, key_in, value_in, level_mask, grad_out))
    return (layer_out, grad_query, grad_key, grad_value)
```

```python
import functools

import jax
import jax.numpy as jnp
import numpy as np
from jax import lax
from jax.experimental import pallas as pl
from jax.experimental.pallas import tpu as pltpu
from jax.sharding import PartitionSpec as P

MESH = pl.DeviceIdType.MESH
HD = 128
F32 = jnp.float32
BF16 = jnp.bfloat16
ROOT_HALF = float(np.float32(2.0**-0.5))


def tier_scale(tier):
    return 1.0 if tier == 0 else float(np.float32(2.0 ** (-(tier - 1) / 2.0)))


def nn(a, b):
    return lax.dot_general(a, b, (((1,), (0,)), ((), ())), preferred_element_type=F32)


def nt(a, b):
    return lax.dot_general(a, b, (((1,), (1,)), ((), ())), preferred_element_type=F32)


def tn(a, b):
    return lax.dot_general(a, b, (((0,), (0,)), ((), ())), preferred_element_type=F32)


def kernel(
    n_seq, heads, length, half_d,
    q_hbm, k_hbm, v_hbm, m_hbm, w_hbm, go_hbm,
    lay_hbm, gq_hbm, gk_hbm, gv_hbm,
    qv, kv, vv, mv, wv, go, gop, wp,
    blend, mb, gacc, gm, state, fr, agg, reach, out, br, total,
    lo, ql, kl, vl, mix, mixp, lay, gq, gk, gv,
    in_sem, out_sem, hs_send, hs_recv, mx_send, mx_recv, fs, fr_sem, bs, br_sem,
):
    n = lax.axis_index("seq")
    core = lax.axis_index("head")
    other = 1 - core
    span = n_seq.bit_length() - 1
    tiers = length.bit_length()
    half = length // 2
    r = lax.rem(n, 4)
    up = [lax.rem(n >> j, 2) for j in range(span)]
    nxt = [lax.rem((n + 1) >> j, 2) for j in range(span)]
    last = n == n_seq - 1
    pending = []

    barrier = pltpu.get_barrier_semaphore()
    dists = (1, n_seq - 1, 2, n_seq - 2, 4, n_seq - 4)
    pl.semaphore_signal(barrier, inc=1, device_id={"head": other}, device_id_type=MESH)
    for d in dists:
        pl.semaphore_signal(
            barrier, inc=1, device_id={"seq": lax.rem(n + d, n_seq)}, device_id_type=MESH
        )

    loads = [
        pltpu.make_async_copy(src, dst, in_sem.at[i])
        for i, (src, dst) in enumerate(
            ((k_hbm.at[0], kv), (v_hbm.at[0], vv), (go_hbm.at[0], go), (w_hbm, wv),
             (m_hbm.at[0], mv), (q_hbm.at[0], qv))
        )
    ]
    for load in loads:
        load.start()
    loads[0].wait()
    loads[1].wait()

    def cols(h):
        return pl.ds(pl.multiple_of(h * HD, HD), HD)

    def state_body(h, carry):
        s = tn(kv[:, cols(h)], vv[:, cols(h)])
        state[h] = s
        agg[h] = s.astype(BF16)
        return carry

    lax.fori_loop(0, heads, state_body, 0)
    loads[2].wait()
    loads[3].wait()

    pl.semaphore_wait(barrier, 1 + len(dists))

    own_cols = pl.ds(pl.multiple_of(core * half_d, HD), half_d)
    other_cols = pl.ds(pl.multiple_of(other * half_d, HD), half_d)

    def to_core(src, dst, i):
        return pltpu.make_async_remote_copy(
            src_ref=src, dst_ref=dst, send_sem=hs_send.at[i], recv_sem=hs_recv.at[i],
            device_id={"head": other}, device_id_type=MESH,
        )

    go_copy = to_core(go, gop, 0)
    w_copy = to_core(wv.at[:, other_cols], wp, 1)
    go_copy.start()

    def fmsg(level, which, c, src, dist):
        return pltpu.make_async_remote_copy(
            src_ref=src, dst_ref=fr.at[level, c], send_sem=fs.at[level, which, c],
            recv_sem=fr_sem.at[level, c], device_id={"seq": n + dist}, device_id_type=MESH,
        )

    def fwait(level, c):
        fmsg(level, 0, c, fr.at[level, c], 0).wait_recv()

    def fsend(level, which, c, src, dist):
        fmsg(level, which, c, src, dist).start()

    def fsent(cond, level, which):
        pending.append(
            (cond, lambda: [fmsg(level, which, c, fr.at[level, c], 0).wait_send() for c in range(heads)])
        )

    def bmsg(level, slot, c, dist):
        return pltpu.make_async_remote_copy(
            src_ref=out.at[level, c], dst_ref=br.at[level, slot, c], send_sem=bs.at[level, c],
            recv_sem=br_sem.at[level, slot, c], device_id={"seq": n - dist}, device_id_type=MESH,
        )

    def bwait(level, slot, c):
        bmsg(level, slot, c, 0).wait_recv()

    even = lax.rem(r, 2) == 0

    @pl.when(even)
    def _():
        for c in range(heads):
            fsend(0, 1, c, agg.at[c], 1)

    w_copy.start()

    def gm_body(source, weight_cols, finish):
        def body(i, carry):
            rows = pl.ds(pl.multiple_of(lax.rem(i, 2) * half, half), half)
            wide = heads * HD // 2
            feats = pl.ds(pl.multiple_of(i // 2 * wide, wide), wide)
            part = nt(source[rows, :], wv[feats, weight_cols])
            if finish:
                gm[rows, feats] = (gacc[rows, feats] + part).astype(BF16)
            else:
                gacc[rows, feats] = part
            return carry

        lax.fori_loop(0, 4, body, 0)

    gm_body(go, own_cols, False)

    @pl.when(r == 1)
    def _():
        for c in range(heads):
            fwait(0, c)
            agg[c] = (state[c] + fr[0, c].astype(F32)).astype(BF16)
            fsend(1, 0, c, agg.at[c], 2)
            fsend(1, 1, c, agg.at[c], 1)

    @pl.when(r == 3)
    def _():
        for c in range(heads):
            fwait(0, c)
            state[c] = state[c] + fr[0, c].astype(F32)

    loads[4].wait()
    loads[5].wait()

    for j in range(span):
        mb[j] = jnp.broadcast_to(mv[:, tiers + j : tiers + j + 1].astype(F32), (length, HD)).astype(BF16)

    go_copy.wait_recv()
    gm_body(gop, other_cols, True)

    def source_of(level):
        return jnp.logical_and(nxt[level] == 1, up[level] == 0)

    @pl.when(r == 3)
    def _():
        first = source_of(2)
        for c in range(heads):
            fwait(1, c)
            tot = state[c] + fr[1, c].astype(F32)
            state[c] = tot
            agg[c] = tot.astype(BF16)

            @pl.when(first)
            def _():
                fsend(2, 0, c, agg.at[c], 4)
                fsend(2, 1, c, agg.at[c], 1)

    def halves(j):
        odd = (tiers + j - 1) % 2
        return odd, 2.0 ** (-((tiers + j - 1 - odd) // 2))

    def reach_body(h, carry):
        q = qv[:, cols(h)]
        qs = (q.astype(F32) * ROOT_HALF).astype(BF16)
        g = gm[:, cols(h)]
        for j in range(span):
            odd, whole = halves(j)

            @pl.when(up[j] == 1)
            def _():
                s = tn(qs if odd else q, mb[j] * g) * whole
                reach[j, h] = s
                out[j, h] = s.astype(BF16)

        return carry

    lax.fori_loop(0, heads, reach_body, 0)

    def bsent(cond, level):
        pending.append((cond, lambda: [bmsg(level, 0, c, 0).wait_send() for c in range(heads)]))

    high = list(range(span - 1, 1, -1))
    for j in high:

        @pl.when(jnp.logical_and(r == 2, up[j] == 1))
        def _():
            for c in range(heads):
                bmsg(j, 2, c, 1).start()

        @pl.when(last)
        def _():
            for c in range(heads):
                bmsg(j, 1, c, 4).start()

    @pl.when(r == 2)
    def _():
        for c in range(heads):
            bmsg(1, 0, c, 1).start()

    @pl.when(last)
    def _():
        for c in range(heads):
            bmsg(1, 1, c, 2).start()
        for c in range(heads):
            bmsg(0, 0, c, 1).start()

    for j in range(span):
        bsent(up[j] == 1, j)

    def blend_block(rows, levels):
        t = lax.broadcasted_iota(jnp.int32, (half, half), 0)
        s = lax.broadcasted_iota(jnp.int32, (half, half), 1)
        spread = jnp.bitwise_xor(t, s)

        def column(level):
            return mv[rows, level : level + 1].astype(F32) * tier_scale(level)

        value = jnp.broadcast_to(column(0), (half, half))
        for level in range(1, levels):
            value = jnp.where(spread >= 1 << (level - 1), column(level), value)
        return jnp.where(s <= t, value, 0.0)

    top, low = pl.ds(0, half), pl.ds(half, half)
    blend[0] = blend_block(top, tiers - 1)
    blend[1] = blend_block(low, tiers - 1)
    blend[2] = jnp.broadcast_to(
        mv[low, tiers - 1 : tiers].astype(F32) * tier_scale(tiers - 1), (half, half)
    )

    def forward_step(j):
        for c in range(heads):
            fwait(j, c)

            @pl.when(r == 3)
            def _():
                @pl.when(nxt[j] == 1)
                def _():
                    fsend(j, 0, c, fr.at[j, c], 4)
                    fsend(j, 1, c, fr.at[j, c], 1)

                if j + 1 < span:

                    @pl.when(nxt[j] == 0)
                    def _():
                        tot = state[c] + fr[j, c].astype(F32)
                        state[c] = tot
                        agg[c] = tot.astype(BF16)

                        @pl.when(source_of(j + 1))
                        def _():
                            fsend(j + 1, 0, c, agg.at[c], 4)
                            fsend(j + 1, 1, c, agg.at[c], 1)

            @pl.when(r < 2)
            def _():
                fsend(j, 1, c, fr.at[j, c], 1)

    def when_forward(j, mine):
        @pl.when(jnp.logical_and(up[j] == 1, mine))
        def _():
            forward_step(j)

    def chain_step(j, position, slot):
        @pl.when(jnp.logical_and(up[j] == 1, r == position))
        def _():
            for c in range(heads):
                bwait(j, 2, c)
                out[j, c] = (reach[j, c] + br[j, 2, c].astype(F32)).astype(BF16)
                bmsg(j, slot, c, 1).start()

    def down(level):
        return {0: (0, 1), 1: (1, 2)}.get(level, (1, 4))

    def back_step(j):
        @pl.when(jnp.logical_and(r == 3, nxt[j] == 1))
        def _():
            @pl.when(up[j] == 1)
            def _():
                for c in range(heads):
                    bwait(j, 0, c)
                    bwait(j, 1, c)
                    tot = br[j, 0, c].astype(F32) + br[j, 1, c].astype(F32)
                    out[j, c] = (reach[j, c] + tot).astype(BF16)
                    bmsg(j, 1, c, 4).start()

            @pl.when(up[j] == 0)
            def _():
                for c in range(heads):
                    bwait(j, 0, c)
                    bwait(j, 1, c)
                    tot = br[j, 0, c].astype(F32) + br[j, 1, c].astype(F32)
                    total[c] = tot
                    out[j - 1, c] = (reach[j - 1, c] + tot).astype(BF16)
                    slot, dist = down(j - 1)
                    bmsg(j - 1, slot, c, dist).start()
                for level in range(j - 2, -1, -1):
                    slot, dist = down(level)
                    for c in range(heads):
                        out[level, c] = (reach[level, c] + total[c]).astype(BF16)
                        bmsg(level, slot, c, dist).start()

    def local_head(h):
        def parts(ref):
            return ref[top, cols(h)], ref[low, cols(h)]

        qa, qb = parts(qv)
        ka, kb = parts(kv)
        va, vb = parts(vv)
        ga, gb = parts(gm)
        paa = (nt(qa, ka) * blend[0]).astype(BF16)
        pba = (nt(qb, ka) * blend[2]).astype(BF16)
        pbb = (nt(qb, kb) * blend[1]).astype(BF16)
        lo[top, cols(h)] = nn(paa, va)
        lo[low, cols(h)] = nn(pba, va) + nn(pbb, vb)
        vl[top, cols(h)] = tn(paa, ga) + tn(pba, gb)
        vl[low, cols(h)] = tn(pbb, gb)
        daa = (nt(ga, va) * blend[0]).astype(BF16)
        dba = (nt(gb, va) * blend[2]).astype(BF16)
        dbb = (nt(gb, vb) * blend[1]).astype(BF16)
        ql[top, cols(h)] = nn(daa, ka)
        ql[low, cols(h)] = nn(dba, ka) + nn(dbb, kb)
        kl[top, cols(h)] = tn(daa, qa) + tn(dba, qb)
        kl[low, cols(h)] = tn(dbb, qb)

    busy = r != 2

    def local_body(i, carry):
        local_head(i)

        @pl.when(i == 0)
        def _():
            when_forward(2, busy)
            for j in high:
                chain_step(j, 1, 2)
            for j in high:
                chain_step(j, 0, 0)

        @pl.when(i == 2)
        def _():
            for j in range(3, span - 1):
                when_forward(j, busy)

        return carry

    lax.fori_loop(0, heads, local_body, 0)
    for j in high:
        back_step(j)
    when_forward(span - 1, busy)

    @pl.when(r == 1)
    def _():
        for c in range(heads):
            bwait(1, 0, c)
            bwait(1, 1, c)
            tot = br[1, 0, c].astype(F32) + br[1, 1, c].astype(F32)
            total[c] = tot
            out[0, c] = (reach[0, c] + tot).astype(BF16)
            bmsg(0, 0, c, 1).start()

    @pl.when(r == 2)
    def _():
        for j in range(1, span):

            @pl.when(up[j] == 1)
            def _():
                for c in range(heads):
                    fwait(j, c)

    for j in range(span):

        @pl.when(up[j] == 0)
        def _():
            fr[j] = jnp.zeros(fr.shape[1:], BF16)

    def mix_copy(h):
        return pltpu.make_async_remote_copy(
            src_ref=mix.at[:, cols(h)], dst_ref=mixp.at[:, cols(h)], send_sem=mx_send.at[h],
            recv_sem=mx_recv.at[h], device_id={"head": other}, device_id_type=MESH,
        )

    def far_body(h, carry):
        q = qv[:, cols(h)]
        qs = (q.astype(F32) * ROOT_HALF).astype(BF16)
        g = gm[:, cols(h)]
        mixed = lo[:, cols(h)]
        query = ql[:, cols(h)]
        for j in range(span):
            odd, whole = halves(j)
            mask = mb[j]
            st = fr[j, h]
            mixed = mixed + nn((qs if odd else q) * mask, st) * whole
            query = query + nt(mask * g, st) * tier_scale(tiers + j)
        mix[:, cols(h)] = mixed.astype(BF16)
        gq[:, cols(h)] = query.astype(BF16)
        mix_copy(h).start()
        return carry

    lax.fori_loop(0, heads, far_body, 0)

    stores = [
        pltpu.make_async_copy(src, dst, out_sem.at[i])
        for i, (src, dst) in enumerate(((gq, gq_hbm.at[0]), (gk, gk_hbm.at[0]), (gv, gv_hbm.at[0]), (lay, lay_hbm.at[0])))
    ]
    stores[0].start()

    w_copy.wait_recv()
    for h in range(heads):
        mix_copy(h).wait_recv()

    tile = 256

    def layer_body(i, carry):
        at = pl.multiple_of(i * tile, tile)
        here = pl.ds(pl.multiple_of(core * half_d + at, HD), tile)
        there = pl.ds(at, tile)
        lay[:, there] = (nn(mix[...], wv[:, here]) + nn(mixp[...], wp[:, there])).astype(BF16)
        return carry

    lax.fori_loop(0, half_d // tile, layer_body, 0)
    stores[3].start()

    @pl.when(even)
    def _():
        for c in range(heads):
            bwait(0, 0, c)
            total[c] = br[0, 0, c].astype(F32)

    @pl.when(last)
    def _():
        total[...] = jnp.zeros(total.shape, F32)

    def back_body(h, carry):
        back = total[h].astype(BF16)
        gk[:, cols(h)] = (kl[:, cols(h)] + nt(vv[:, cols(h)], back)).astype(BF16)
        gv[:, cols(h)] = (vl[:, cols(h)] + nn(kv[:, cols(h)], back)).astype(BF16)
        return carry

    lax.fori_loop(0, heads, back_body, 0)
    stores[1].start()
    stores[2].start()

    fsent(even, 0, 1)
    fsent(r == 1, 1, 0)
    fsent(r == 1, 1, 1)
    for j in range(2, span):
        sends = jnp.logical_and(r == 3, nxt[j] == 1)
        fsent(sends, j, 0)
        fsent(jnp.logical_or(sends, jnp.logical_and(r < 2, up[j] == 1)), j, 1)
    for cond, wait in pending:

        @pl.when(cond)
        def _():
            wait()

    go_copy.wait_send()
    w_copy.wait_send()
    for h in range(heads):
        mix_copy(h).wait_send()
    for store in stores:
        store.wait()


def on_device(query_in, key_in, value_in, level_mask, out_weight, grad_out):
    n_seq = lax.axis_size("seq")
    _, length, width = query_in.shape
    heads = width // HD
    half_d = grad_out.shape[2]
    span = n_seq.bit_length() - 1
    half = length // 2
    wide = lambda dtype: pltpu.VMEM((length, width), dtype)
    any_spec = pl.BlockSpec(memory_space=pl.ANY)
    dma = lambda *shape: pltpu.SemaphoreType.DMA(shape)
    layer, gq, gk, gv = pl.pallas_call(
        functools.partial(kernel, n_seq, heads, length, half_d),
        out_shape=(
            jax.ShapeDtypeStruct(grad_out.shape, BF16),
            jax.ShapeDtypeStruct(query_in.shape, BF16),
            jax.ShapeDtypeStruct(query_in.shape, BF16),
            jax.ShapeDtypeStruct(query_in.shape, BF16),
        ),
        in_specs=[any_spec] * 6,
        out_specs=(any_spec,) * 4,
        scratch_shapes=[
            wide(BF16), wide(BF16), wide(BF16),
            pltpu.VMEM(level_mask.shape[1:], jnp.int32),
            pltpu.VMEM(out_weight.shape, BF16),
            pltpu.VMEM((length, half_d), BF16),
            pltpu.VMEM((length, half_d), BF16),
            pltpu.VMEM((width, half_d), BF16),
            pltpu.VMEM((3, half, half), F32),
            pltpu.VMEM((span, length, HD), BF16),
            wide(F32), wide(BF16),
            pltpu.VMEM((heads, HD, HD), F32),
            pltpu.VMEM((span, heads, HD, HD), BF16),
            pltpu.VMEM((heads, HD, HD), BF16),
            pltpu.VMEM((span, heads, HD, HD), F32),
            pltpu.VMEM((span, heads, HD, HD), BF16),
            pltpu.VMEM((span, 3, heads, HD, HD), BF16),
            pltpu.VMEM((heads, HD, HD), F32),
            wide(F32), wide(F32), wide(F32), wide(F32),
            wide(BF16), wide(BF16),
            pltpu.VMEM((length, half_d), BF16),
            wide(BF16), wide(BF16), wide(BF16),
            dma(6), dma(4), dma(2), dma(2), dma(heads), dma(heads),
            dma(span, 2, heads), dma(span, heads), dma(span, heads), dma(span, 3, heads),
        ],
        compiler_params=pltpu.CompilerParams(collective_id=0, has_side_effects=True),
        name="log_linear",
    )(query_in, key_in, value_in, level_mask, out_weight, grad_out)
    return layer, gq, gk, gv


def solution(mesh):
    return jax.shard_map(
        on_device,
        mesh=mesh,
        in_specs=(
            P(("groups", "batch"), "seq", "head"),
            P(("groups", "batch"), "seq", "head"),
            P(("groups", "batch"), "seq", "head"),
            P(("groups", "batch"), "seq", None),
            P("head", None),
            P(("groups", "batch"), "seq", "head"),
        ),
        out_specs=(
            P(("groups", "batch"), "seq", "head"),
            P(("groups", "batch"), "seq", "head"),
            P(("groups", "batch"), "seq", "head"),
            P(("groups", "batch"), "seq", "head"),
        ),
        check_vma=False,
    )
```

```python
import functools

import jax
import jax.numpy as jnp
import numpy as np
from jax import lax
from jax.experimental import pallas as pl
from jax.experimental.pallas import tpu as pltpu
from jax.sharding import PartitionSpec as P

MESH = pl.DeviceIdType.MESH
HD = 128
F32 = jnp.float32
BF16 = jnp.bfloat16
ROOT_HALF = float(np.float32(2.0**-0.5))


def tier_scale(tier):
    return 1.0 if tier == 0 else float(np.float32(2.0 ** (-(tier - 1) / 2.0)))


def nn(a, b):
    return lax.dot_general(a, b, (((1,), (0,)), ((), ())), preferred_element_type=F32)


def nt(a, b):
    return lax.dot_general(a, b, (((1,), (1,)), ((), ())), preferred_element_type=F32)


def tn(a, b):
    return lax.dot_general(a, b, (((0,), (0,)), ((), ())), preferred_element_type=F32)


def kernel(
    n_seq, heads, length, half_d,
    q_hbm, k_hbm, v_hbm, m_hbm, w_hbm, go_hbm,
    lay_hbm, gq_hbm, gk_hbm, gv_hbm,
    qv, kv, vv, mt, mv, wv, go, gop, wp,
    blend, mb, gacc, gm, state, fr, agg, reach, out, br, total,
    lo, ql, kl, vl, mix, mixp, lay, gq, gk, gv, ur, qt,
    in_sem, out_sem, hs_send, hs_recv, mx_send, mx_recv, fs, fr_sem, bs, br_sem, us, ur_sem, ready,
):
    n = lax.axis_index("seq")
    core = lax.axis_index("head")
    other = 1 - core
    span = n_seq.bit_length() - 1
    tiers = length.bit_length()
    half = length // 2
    r = lax.rem(n, 4)
    up = [lax.rem(n >> j, 2) for j in range(span)]
    nxt = [lax.rem((n + 1) >> j, 2) for j in range(span)]
    top_level = span - 1
    n_half = n_seq // 2
    upper = up[top_level] == 1
    inner = lax.rem(n, n_half)
    after = [lax.rem((inner + 1) >> j, 2) for j in range(top_level)]
    last = inner == n_half - 1
    end = n == n_seq - 1
    pending = []
    slots = m_hbm.shape[1]

    barrier = pltpu.get_barrier_semaphore()
    dists = (1, 2, 4)
    pl.semaphore_signal(barrier, inc=1, device_id={"head": other}, device_id_type=MESH)
    for d in dists:

        @pl.when(n + d < n_seq)
        def _():
            pl.semaphore_signal(barrier, inc=1, device_id={"seq": n + d}, device_id_type=MESH)

    for first in (0, 3):

        @pl.when(n == first)
        def _():
            pl.semaphore_signal(barrier, inc=1, device_id={"seq": n_seq - 1}, device_id_type=MESH)

    loads = [
        pltpu.make_async_copy(src, dst, in_sem.at[i])
        for i, (src, dst) in enumerate(
            ((k_hbm.at[0], kv), (v_hbm.at[0], vv), (go_hbm.at[0], go), (w_hbm, wv),
             (m_hbm.at[0], mt.at[pl.ds(0, slots)]), (q_hbm.at[0], qv))
        )
    ]
    for i in (5, 4, 2, 3, 0, 1):
        loads[i].start()

    one = lambda cond: cond.astype(jnp.int32)
    pl.semaphore_wait(barrier, 1 + one(n >= 1) + one(n >= 2) + one(n >= 4) + 2 * one(end))

    own_cols = pl.ds(pl.multiple_of(core * half_d, HD), half_d)
    other_cols = pl.ds(pl.multiple_of(other * half_d, HD), half_d)

    def to_core(src, dst, i):
        return pltpu.make_async_remote_copy(
            src_ref=src, dst_ref=dst, send_sem=hs_send.at[i], recv_sem=hs_recv.at[i],
            device_id={"head": other}, device_id_type=MESH,
        )

    go_copy = to_core(go_hbm.at[0], gop, 0)
    w_copy = to_core(w_hbm.at[:, other_cols], wp, 1)
    go_copy.start()
    w_copy.start()
    for d in dists:

        @pl.when(n >= d)
        def _():
            pl.semaphore_signal(ready, inc=1, device_id={"seq": n - d}, device_id_type=MESH)

    def cols(h):
        return pl.ds(pl.multiple_of(h * HD, HD), HD)

    loads[5].wait()
    loads[4].wait()
    mt[slots:, :] = jnp.zeros((HD - slots, length), jnp.int32)
    mv[...] = mt[...].astype(F32).T
    for j in range(span):
        mb[j] = jnp.broadcast_to(mv[:, tiers + j : tiers + j + 1], (length, HD)).astype(BF16)

    def turn_body(h, carry):
        q = qv[:, cols(h)].astype(F32)
        qt[0, h] = q.T.astype(BF16)
        qt[1, h] = (q * ROOT_HALF).T.astype(BF16)
        return carry

    lax.fori_loop(0, heads, turn_body, 0)

    def gm_body(i, carry):
        rows = pl.ds(pl.multiple_of(lax.rem(i, 2) * half, half), half)
        wide = heads * HD // 2
        feats = pl.ds(pl.multiple_of(i // 2 * wide, wide), wide)
        gacc[rows, feats] = nt(go[rows, :], wv[feats, own_cols])
        return carry

    loads[2].wait()
    loads[3].wait()
    lax.fori_loop(0, 4, gm_body, 0)

    def fmsg(level, which, c, src, dist):
        return pltpu.make_async_remote_copy(
            src_ref=src, dst_ref=fr.at[level, c], send_sem=fs.at[level, which, c],
            recv_sem=fr_sem.at[level, c], device_id={"seq": n + dist}, device_id_type=MESH,
        )

    def fwait(level, c):
        fmsg(level, 0, c, fr.at[level, c], 0).wait_recv()

    def fsend(level, which, c, src, dist):
        fmsg(level, which, c, src, dist).start()

    def fsent(cond, level, which):
        pending.append(
            (cond, lambda: [fmsg(level, which, c, fr.at[level, c], 0).wait_send() for c in range(heads)])
        )

    def bmsg(level, slot, c, dist):
        return pltpu.make_async_remote_copy(
            src_ref=out.at[level, c], dst_ref=br.at[level, slot, c], send_sem=bs.at[level, c],
            recv_sem=br_sem.at[level, slot, c], device_id={"seq": n - dist}, device_id_type=MESH,
        )

    def bwait(level, slot, c):
        bmsg(level, slot, c, 0).wait_recv()

    def umsg(which, slot, c, dist, src=None):
        return pltpu.make_async_remote_copy(
            src_ref=out.at[top_level, c] if src is None else src, dst_ref=ur.at[slot, c],
            send_sem=us.at[which, c], recv_sem=ur_sem.at[slot, c],
            device_id={"seq": lax.rem(n + dist, n_seq)}, device_id_type=MESH,
        )

    def uwait(slot, c):
        umsg(0, slot, c, 0).wait_recv()

    even = lax.rem(r, 2) == 0

    def state_body(h, carry):
        s = tn(kv[:, cols(h)], vv[:, cols(h)])
        state[h] = s
        agg[h] = s.astype(BF16)
        return carry

    def upper_in():
        @pl.when(jnp.logical_not(end))
        def _():
            pl.semaphore_wait(
                ready, one(n + 1 < n_seq) + one(n + 2 < n_seq) + one(n + 4 < n_seq)
            )

    def open_forward():
        lax.fori_loop(0, heads, state_body, 0)

        @pl.when(jnp.logical_not(upper))
        def _():
            upper_in()

        @pl.when(even)
        def _():
            for c in range(heads):
                fsend(0, 1, c, agg.at[c], 1)

    loads[0].wait()
    loads[1].wait()

    @pl.when(n == 0)
    def _():
        open_forward()

    def halves(j):
        odd = (tiers + j - 1) % 2
        return odd, 2.0 ** (-((tiers + j - 1 - odd) // 2))

    def reach_level(j, h, g):
        odd, whole = halves(j)
        s = nn(qt[odd, h], mb[j] * g) * whole
        reach[j, h] = s
        out[j, h] = s.astype(BF16)

    @pl.when(upper)
    def _():
        upper_in()

    go_copy.wait_recv()

    def finish_body(h, carry):
        g = (gacc[:, cols(h)] + nt(gop[...], wv[cols(h), other_cols])).astype(BF16)
        gm[:, cols(h)] = g

        @pl.when(upper)
        def _():
            reach_level(top_level, h, g)

            @pl.when(r == 0)
            def _():
                umsg(0, 0, h, 1).start()

            @pl.when(r == 2)
            def _():
                umsg(0, 1, h, 1).start()

        return carry

    lax.fori_loop(0, heads, finish_body, 0)

    def joined(c, slots_in):
        tot = reach[top_level, c]
        for slot in slots_in:
            uwait(slot, c)
            tot = tot + ur[slot, c].astype(F32)
        return tot

    @pl.when(jnp.logical_and(upper, r == 1))
    def _():
        for c in range(heads):
            out[top_level, c] = joined(c, (0,)).astype(BF16)
            umsg(0, 0, c, 2).start()

    @pl.when(jnp.logical_and(upper, r == 3))
    def _():
        @pl.when(inner == 3)
        def _():
            for c in range(heads):
                out[top_level, c] = joined(c, (0, 1)).astype(BF16)
                umsg(0, 2, c, 4).start()

        @pl.when(jnp.logical_and(inner != 3, jnp.logical_not(end)))
        def _():
            for c in range(heads):
                out[top_level, c] = joined(c, (0, 1, 2)).astype(BF16)
                umsg(0, 2, c, 4).start()

        @pl.when(end)
        def _():
            for c in range(heads):
                out[top_level, c] = joined(c, (0, 1, 2)).astype(BF16)
                umsg(1, 3, c, 1).start()
                umsg(0, 3, c, 4).start()

    def reach_body(h, carry):
        g = gm[:, cols(h)]
        for j in range(top_level):

            @pl.when(up[j] == 1)
            def _():
                reach_level(j, h, g)

        return carry

    lax.fori_loop(0, heads, reach_body, 0)

    def bsent(cond, level):
        pending.append((cond, lambda: [bmsg(level, 0, c, 0).wait_send() for c in range(heads)]))

    high = list(range(top_level - 1, 1, -1))
    for j in high:

        @pl.when(jnp.logical_and(r == 2, up[j] == 1))
        def _():
            for c in range(heads):
                bmsg(j, 2, c, 1).start()

        @pl.when(last)
        def _():
            for c in range(heads):
                bmsg(j, 1, c, 4).start()

    @pl.when(r == 2)
    def _():
        for c in range(heads):
            bmsg(1, 0, c, 1).start()

    @pl.when(last)
    def _():
        for c in range(heads):
            bmsg(1, 1, c, 2).start()
        for c in range(heads):
            bmsg(0, 0, c, 1).start()

    for j in range(top_level):
        early = False
        if 1 <= j < top_level - 1:
            early = jnp.logical_and(jnp.logical_and(r == 3, after[j + 1] == 1), up[j + 1] == 0)
        bsent(jnp.logical_and(up[j] == 1, jnp.logical_not(early)), j)

    def chain_step(j, position, slot):
        @pl.when(jnp.logical_and(up[j] == 1, r == position))
        def _():
            for c in range(heads):
                bwait(j, 2, c)
                out[j, c] = (reach[j, c] + br[j, 2, c].astype(F32)).astype(BF16)
                bmsg(j, slot, c, 1).start()

    @pl.when(n != 0)
    def _():
        open_forward()

    for j in high:
        chain_step(j, 1, 2)
    for j in high:
        chain_step(j, 0, 0)

    def blend_block(rows, levels):
        t = lax.broadcasted_iota(jnp.int32, (half, half), 0)
        s = lax.broadcasted_iota(jnp.int32, (half, half), 1)
        spread = jnp.bitwise_xor(t, s)

        def column(level):
            return mv[rows, level : level + 1] * tier_scale(level)

        value = jnp.broadcast_to(column(0), (half, half))
        for level in range(1, levels):
            value = jnp.where(spread >= 1 << (level - 1), column(level), value)
        return jnp.where(s <= t, value, 0.0)

    top, low = pl.ds(0, half), pl.ds(half, half)
    blend[0] = blend_block(top, tiers - 1)
    blend[1] = blend_block(low, tiers - 1)
    blend[2] = jnp.broadcast_to(
        mv[low, tiers - 1 : tiers] * tier_scale(tiers - 1), (half, half)
    )

    def forward_step(j):
        for c in range(heads):
            fwait(j, c)

            @pl.when(r == 3)
            def _():
                @pl.when(nxt[j] == 1)
                def _():
                    fsend(j, 0, c, fr.at[j, c], 4)
                    fsend(j, 1, c, fr.at[j, c], 1)

                if j + 1 < span:

                    @pl.when(nxt[j] == 0)
                    def _():
                        tot = state[c] + fr[j, c].astype(F32)
                        state[c] = tot
                        agg[c] = tot.astype(BF16)

                        @pl.when(source_of(j + 1))
                        def _():
                            fsend(j + 1, 0, c, agg.at[c], 4)
                            fsend(j + 1, 1, c, agg.at[c], 1)

            @pl.when(r < 2)
            def _():
                fsend(j, 1, c, fr.at[j, c], 1)

    def when_forward(j, mine):
        @pl.when(jnp.logical_and(up[j] == 1, mine))
        def _():
            forward_step(j)

    def down(level):
        return {0: (0, 1), 1: (1, 2)}.get(level, (1, 4))

    def back_step(j):
        @pl.when(jnp.logical_and(r == 3, after[j] == 1))
        def _():
            @pl.when(up[j] == 1)
            def _():
                for c in range(heads):
                    bwait(j, 0, c)
                    bwait(j, 1, c)
                    tot = br[j, 0, c].astype(F32) + br[j, 1, c].astype(F32)
                    out[j, c] = (reach[j, c] + tot).astype(BF16)
                    bmsg(j, 1, c, 4).start()

            @pl.when(up[j] == 0)
            def _():
                for c in range(heads):
                    bwait(j, 0, c)
                    bwait(j, 1, c)
                    tot = br[j, 0, c].astype(F32) + br[j, 1, c].astype(F32)
                    total[c] = tot
                    out[j - 1, c] = (reach[j - 1, c] + tot).astype(BF16)
                    slot, dist = down(j - 1)
                    bmsg(j - 1, slot, c, dist).start()
                for c in range(heads):
                    bmsg(j - 1, slot, c, dist).wait_send()
                for level in range(j - 2, -1, -1):
                    slot, dist = down(level)
                    for c in range(heads):
                        out[level, c] = (reach[level, c] + total[c]).astype(BF16)
                        bmsg(level, slot, c, dist).start()

    def local_head(h):
        def parts(ref):
            return ref[top, cols(h)], ref[low, cols(h)]

        qa, qb = parts(qv)
        ka, kb = parts(kv)
        va, vb = parts(vv)
        ga, gb = parts(gm)
        paa = (nt(qa, ka) * blend[0]).astype(BF16)
        pba = (nt(qb, ka) * blend[2]).astype(BF16)
        pbb = (nt(qb, kb) * blend[1]).astype(BF16)
        lo[top, cols(h)] = nn(paa, va)
        lo[low, cols(h)] = nn(pba, va) + nn(pbb, vb)
        vl[top, cols(h)] = tn(paa, ga) + tn(pba, gb)
        vl[low, cols(h)] = tn(pbb, gb)
        daa = (nt(ga, va) * blend[0]).astype(BF16)
        dba = (nt(gb, va) * blend[2]).astype(BF16)
        dbb = (nt(gb, vb) * blend[1]).astype(BF16)
        ql[top, cols(h)] = nn(daa, ka)
        ql[low, cols(h)] = nn(dba, ka) + nn(dbb, kb)
        kl[top, cols(h)] = tn(daa, qa) + tn(dba, qb)
        kl[low, cols(h)] = tn(dbb, qb)

    busy = r != 2

    def local_body(i, carry):
        local_head(i)
        return carry

    lax.fori_loop(0, heads, local_body, 0)

    @pl.when(r == 1)
    def _():
        for c in range(heads):
            fwait(0, c)
            agg[c] = (state[c] + fr[0, c].astype(F32)).astype(BF16)
            fsend(1, 0, c, agg.at[c], 2)
            fsend(1, 1, c, agg.at[c], 1)

    def source_of(level):
        return jnp.logical_and(nxt[level] == 1, up[level] == 0)

    @pl.when(r == 3)
    def _():
        first = source_of(2)
        for c in range(heads):
            fwait(0, c)
            state[c] = state[c] + fr[0, c].astype(F32)
        for c in range(heads):
            fwait(1, c)
            tot = state[c] + fr[1, c].astype(F32)
            state[c] = tot
            agg[c] = tot.astype(BF16)

            @pl.when(first)
            def _():
                fsend(2, 0, c, agg.at[c], 4)
                fsend(2, 1, c, agg.at[c], 1)

    for j in high:
        back_step(j)

    @pl.when(r == 1)
    def _():
        for c in range(heads):
            bwait(1, 0, c)
            bwait(1, 1, c)
            tot = br[1, 0, c].astype(F32) + br[1, 1, c].astype(F32)
            total[c] = tot
            out[0, c] = (reach[0, c] + tot).astype(BF16)
            bmsg(0, 0, c, 1).start()

    when_forward(2, busy)
    for j in range(3, top_level):
        when_forward(j, busy)
    when_forward(top_level, busy)

    @pl.when(r == 2)
    def _():
        for j in range(1, span):

            @pl.when(up[j] == 1)
            def _():
                for c in range(heads):
                    fwait(j, c)

    for j in range(span):

        @pl.when(up[j] == 0)
        def _():
            fr[j] = jnp.zeros(fr.shape[1:], BF16)

    def mix_copy(h):
        return pltpu.make_async_remote_copy(
            src_ref=mix.at[:, cols(h)], dst_ref=mixp.at[:, cols(h)], send_sem=mx_send.at[h],
            recv_sem=mx_recv.at[h], device_id={"head": other}, device_id_type=MESH,
        )

    def far_body(h, carry):
        q = qv[:, cols(h)]
        qs = (q.astype(F32) * ROOT_HALF).astype(BF16)
        g = gm[:, cols(h)]
        mixed = lo[:, cols(h)]
        query = ql[:, cols(h)]
        for j in range(span):
            odd, whole = halves(j)
            mask = mb[j]
            st = fr[j, h]
            mixed = mixed + nn((qs if odd else q) * mask, st) * whole
            query = query + nt(mask * g, st) * tier_scale(tiers + j)
        mix[:, cols(h)] = mixed.astype(BF16)
        gq[:, cols(h)] = query.astype(BF16)
        mix_copy(h).start()
        return carry

    lax.fori_loop(0, heads, far_body, 0)

    stores = [
        pltpu.make_async_copy(src, dst, out_sem.at[i])
        for i, (src, dst) in enumerate(((gq, gq_hbm.at[0]), (gk, gk_hbm.at[0]), (gv, gv_hbm.at[0]), (lay, lay_hbm.at[0])))
    ]
    stores[0].start()

    w_copy.wait_recv()
    for h in range(heads):
        mix_copy(h).wait_recv()

    tile = 256

    def layer_body(i, carry):
        at = pl.multiple_of(i * tile, tile)
        here = pl.ds(pl.multiple_of(core * half_d + at, HD), tile)
        there = pl.ds(at, tile)
        lay[:, there] = (nn(mix[...], wv[:, here]) + nn(mixp[...], wp[:, there])).astype(BF16)
        return carry

    lax.fori_loop(0, half_d // tile, layer_body, 0)
    stores[3].start()

    @pl.when(even)
    def _():
        for c in range(heads):
            bwait(0, 0, c)
            total[c] = br[0, 0, c].astype(F32)

    @pl.when(last)
    def _():
        total[...] = jnp.zeros(total.shape, F32)

    def back_body(h, carry):
        @pl.when(jnp.logical_not(upper))
        def _():
            uwait(3, h)

            @pl.when(jnp.logical_and(r == 3, jnp.logical_not(last)))
            def _():
                umsg(0, 3, h, 4, ur.at[3, h]).start()

            @pl.when(jnp.logical_or(r < 2, jnp.logical_and(r == 3, jnp.logical_not(last))))
            def _():
                umsg(1, 3, h, 1, ur.at[3, h]).start()

            total[h] = total[h] + ur[3, h].astype(F32)

        back = total[h].astype(BF16)
        gk[:, cols(h)] = (kl[:, cols(h)] + nt(vv[:, cols(h)], back)).astype(BF16)
        gv[:, cols(h)] = (vl[:, cols(h)] + nn(kv[:, cols(h)], back)).astype(BF16)
        return carry

    lax.fori_loop(0, heads, back_body, 0)
    stores[1].start()
    stores[2].start()

    fsent(even, 0, 1)
    fsent(r == 1, 1, 0)
    fsent(r == 1, 1, 1)
    for j in range(2, span):
        sends = jnp.logical_and(r == 3, nxt[j] == 1)
        fsent(sends, j, 0)
        fsent(jnp.logical_or(sends, jnp.logical_and(r < 2, up[j] == 1)), j, 1)

    def usent(cond, which):
        pending.append((cond, lambda: [umsg(which, 3, c, 0).wait_send() for c in range(heads)]))

    lower_hop = jnp.logical_and(jnp.logical_not(upper), jnp.logical_and(r == 3, jnp.logical_not(last)))
    usent(jnp.logical_or(upper, lower_hop), 0)
    lower_near = jnp.logical_or(lower_hop, jnp.logical_and(jnp.logical_not(upper), r < 2))
    usent(jnp.logical_or(end, lower_near), 1)
    for cond, wait in pending:

        @pl.when(cond)
        def _():
            wait()

    go_copy.wait_send()
    w_copy.wait_send()
    for h in range(heads):
        mix_copy(h).wait_send()
    for store in stores:
        store.wait()


def on_device(query_in, key_in, value_in, level_mask, out_weight, grad_out):
    n_seq = lax.axis_size("seq")
    _, length, width = query_in.shape
    heads = width // HD
    half_d = grad_out.shape[2]
    span = n_seq.bit_length() - 1
    half = length // 2
    wide = lambda dtype: pltpu.VMEM((length, width), dtype)
    any_spec = pl.BlockSpec(memory_space=pl.ANY)
    dma = lambda *shape: pltpu.SemaphoreType.DMA(shape)
    layer, gq, gk, gv = pl.pallas_call(
        functools.partial(kernel, n_seq, heads, length, half_d),
        out_shape=(
            jax.ShapeDtypeStruct(grad_out.shape, BF16),
            jax.ShapeDtypeStruct(query_in.shape, BF16),
            jax.ShapeDtypeStruct(query_in.shape, BF16),
            jax.ShapeDtypeStruct(query_in.shape, BF16),
        ),
        in_specs=[any_spec] * 6,
        out_specs=(any_spec,) * 4,
        scratch_shapes=[
            wide(BF16), wide(BF16), wide(BF16),
            pltpu.VMEM((HD, length), jnp.int32),
            pltpu.VMEM((length, HD), F32),
            pltpu.VMEM(out_weight.shape, BF16),
            pltpu.VMEM((length, half_d), BF16),
            pltpu.VMEM((length, half_d), BF16),
            pltpu.VMEM((width, half_d), BF16),
            pltpu.VMEM((3, half, half), F32),
            pltpu.VMEM((span, length, HD), BF16),
            wide(F32), wide(BF16),
            pltpu.VMEM((heads, HD, HD), F32),
            pltpu.VMEM((span, heads, HD, HD), BF16),
            pltpu.VMEM((heads, HD, HD), BF16),
            pltpu.VMEM((span, heads, HD, HD), F32),
            pltpu.VMEM((span, heads, HD, HD), BF16),
            pltpu.VMEM((span, 3, heads, HD, HD), BF16),
            pltpu.VMEM((heads, HD, HD), F32),
            wide(F32), wide(F32), wide(F32), wide(F32),
            wide(BF16), wide(BF16),
            pltpu.VMEM((length, half_d), BF16),
            wide(BF16), wide(BF16), wide(BF16),
            pltpu.VMEM((4, heads, HD, HD), BF16),
            pltpu.VMEM((2, heads, HD, length), BF16),
            dma(6), dma(4), dma(2), dma(2), dma(heads), dma(heads),
            dma(span, 2, heads), dma(span, heads), dma(span, heads), dma(span, 3, heads),
            dma(2, heads), dma(4, heads), pltpu.SemaphoreType.REGULAR,
        ],
        compiler_params=pltpu.CompilerParams(collective_id=0, has_side_effects=True),
        name="log_linear",
    )(query_in, key_in, value_in, jnp.swapaxes(level_mask, 1, 2), out_weight, grad_out)
    return layer, gq, gk, gv


def solution(mesh):
    return jax.shard_map(
        on_device,
        mesh=mesh,
        in_specs=(
            P(("groups", "batch"), "seq", "head"),
            P(("groups", "batch"), "seq", "head"),
            P(("groups", "batch"), "seq", "head"),
            P(("groups", "batch"), "seq", None),
            P("head", None),
            P(("groups", "batch"), "seq", "head"),
        ),
        out_specs=(
            P(("groups", "batch"), "seq", "head"),
            P(("groups", "batch"), "seq", "head"),
            P(("groups", "batch"), "seq", "head"),
            P(("groups", "batch"), "seq", "head"),
        ),
        check_vma=False,
    )
```

```python
import functools

import jax
import jax.numpy as jnp
import numpy as np
from jax import lax
from jax.experimental import pallas as pl
from jax.experimental.pallas import tpu as pltpu
from jax.sharding import PartitionSpec as P

MESH = pl.DeviceIdType.MESH
HD = 128
F32 = jnp.float32
BF16 = jnp.bfloat16
ROOT_HALF = float(np.float32(2.0**-0.5))


def tier_scale(tier):
    return 1.0 if tier == 0 else float(np.float32(2.0 ** (-(tier - 1) / 2.0)))


def nn(a, b):
    return lax.dot_general(a, b, (((1,), (0,)), ((), ())), preferred_element_type=F32)


def nt(a, b):
    return lax.dot_general(a, b, (((1,), (1,)), ((), ())), preferred_element_type=F32)


def tn(a, b):
    return lax.dot_general(a, b, (((0,), (0,)), ((), ())), preferred_element_type=F32)


def kernel(
    n_seq, heads, length, half_d,
    q_hbm, k_hbm, v_hbm, m_hbm, w_hbm, go_hbm,
    lay_hbm, gq_hbm, gk_hbm, gv_hbm,
    qv, kv, vv, mt, mv, wv, go, gop, wp,
    blend, mb, gacc, gm, state, fr, agg, reach, out, br, total,
    lo, ql, kl, vl, mix, mixp, lay, gq, gk, gv, ur, qt,
    in_sem, out_sem, hs_send, hs_recv, mx_send, mx_recv, fs, fr_sem, bs, br_sem, us, ur_sem, ready,
):
    n = lax.axis_index("seq")
    core = lax.axis_index("head")
    other = 1 - core
    span = n_seq.bit_length() - 1
    tiers = length.bit_length()
    half = length // 2
    r = lax.rem(n, 4)
    up = [lax.rem(n >> j, 2) for j in range(span)]
    nxt = [lax.rem((n + 1) >> j, 2) for j in range(span)]
    top_level = span - 1
    n_half = n_seq // 2
    upper = up[top_level] == 1
    inner = lax.rem(n, n_half)
    after = [lax.rem((inner + 1) >> j, 2) for j in range(top_level)]
    last = inner == n_half - 1
    end = n == n_seq - 1
    pending = []
    slots = m_hbm.shape[1]

    barrier = pltpu.get_barrier_semaphore()
    dists = (1, 2, 4)
    pl.semaphore_signal(barrier, inc=1, device_id={"head": other}, device_id_type=MESH)
    for d in dists:

        @pl.when(n + d < n_seq)
        def _():
            pl.semaphore_signal(barrier, inc=1, device_id={"seq": n + d}, device_id_type=MESH)

    @pl.when(inner == 7)
    def _():
        for d in (7, 8):
            pl.semaphore_signal(barrier, inc=1, device_id={"seq": n + d}, device_id_type=MESH)

    for first in (0, 3):

        @pl.when(n == first)
        def _():
            pl.semaphore_signal(barrier, inc=1, device_id={"seq": n_seq - 1}, device_id_type=MESH)

    loads = [
        pltpu.make_async_copy(src, dst, in_sem.at[i])
        for i, (src, dst) in enumerate(
            ((k_hbm.at[0], kv), (v_hbm.at[0], vv), (go_hbm.at[0], go), (w_hbm, wv),
             (m_hbm.at[0], mt.at[pl.ds(0, slots)]), (q_hbm.at[0], qv))
        )
    ]
    for i in (5, 4, 2, 3, 0, 1):
        loads[i].start()

    one = lambda cond: cond.astype(jnp.int32)
    pl.semaphore_wait(barrier, 1 + one(n >= 1) + one(n >= 2) + one(n >= 4) + 2 * one(end) + one(inner >= 14))

    own_cols = pl.ds(pl.multiple_of(core * half_d, HD), half_d)
    other_cols = pl.ds(pl.multiple_of(other * half_d, HD), half_d)

    def to_core(src, dst, i):
        return pltpu.make_async_remote_copy(
            src_ref=src, dst_ref=dst, send_sem=hs_send.at[i], recv_sem=hs_recv.at[i],
            device_id={"head": other}, device_id_type=MESH,
        )

    go_copy = to_core(go_hbm.at[0], gop, 0)
    w_copy = to_core(w_hbm.at[:, other_cols], wp, 1)
    go_copy.start()
    w_copy.start()
    for i, d in enumerate(dists):

        @pl.when(n >= d)
        def _():
            pl.semaphore_signal(ready.at[i], inc=1, device_id={"seq": n - d}, device_id_type=MESH)

    @pl.when(end)
    def _():
        pl.semaphore_signal(ready.at[3], inc=1, device_id={"seq": n - 8}, device_id_type=MESH)

    def cols(h):
        return pl.ds(pl.multiple_of(h * HD, HD), HD)

    loads[5].wait()
    loads[4].wait()
    mt[slots:, :] = jnp.zeros((HD - slots, length), jnp.int32)
    mv[...] = mt[...].astype(F32).T
    for j in range(span):
        mb[j] = jnp.broadcast_to(mv[:, tiers + j : tiers + j + 1], (length, HD)).astype(BF16)

    def turn_body(h, carry):
        q = qv[:, cols(h)].astype(F32)
        qt[0, h] = q.T.astype(BF16)
        qt[1, h] = (q * ROOT_HALF).T.astype(BF16)
        return carry

    lax.fori_loop(0, heads, turn_body, 0)

    def gm_body(i, carry):
        rows = pl.ds(pl.multiple_of(lax.rem(i, 2) * half, half), half)
        wide = heads * HD // 2
        feats = pl.ds(pl.multiple_of(i // 2 * wide, wide), wide)
        gacc[rows, feats] = nt(go[rows, :], wv[feats, own_cols])
        return carry

    loads[2].wait()
    loads[3].wait()
    lax.fori_loop(0, 4, gm_body, 0)

    def fmsg(level, which, c, src, dist):
        return pltpu.make_async_remote_copy(
            src_ref=src, dst_ref=fr.at[level, c], send_sem=fs.at[level, which, c],
            recv_sem=fr_sem.at[level, c], device_id={"seq": n + dist}, device_id_type=MESH,
        )

    def fwait(level, c):
        fmsg(level, 0, c, fr.at[level, c], 0).wait_recv()

    def fsend(level, which, c, src, dist):
        fmsg(level, which, c, src, dist).start()

    def fsent(cond, level, which):
        pending.append(
            (cond, lambda: [fmsg(level, which, c, fr.at[level, c], 0).wait_send() for c in range(heads)])
        )

    def bmsg(level, slot, c, dist):
        return pltpu.make_async_remote_copy(
            src_ref=out.at[level, c], dst_ref=br.at[level, slot, c], send_sem=bs.at[level, c],
            recv_sem=br_sem.at[level, slot, c], device_id={"seq": n - dist}, device_id_type=MESH,
        )

    def bwait(level, slot, c):
        bmsg(level, slot, c, 0).wait_recv()

    def umsg(which, slot, c, dist, src=None):
        return pltpu.make_async_remote_copy(
            src_ref=out.at[top_level, c] if src is None else src, dst_ref=ur.at[slot, c],
            send_sem=us.at[which, c], recv_sem=ur_sem.at[slot, c],
            device_id={"seq": lax.rem(n + dist, n_seq)}, device_id_type=MESH,
        )

    def uwait(slot, c):
        umsg(0, slot, c, 0).wait_recv()

    even = lax.rem(r, 2) == 0

    def state_body(h, carry):
        s = tn(kv[:, cols(h)], vv[:, cols(h)])
        state[h] = s
        agg[h] = s.astype(BF16)
        return carry

    soon = (
        jnp.logical_or(upper, r < 2),
        jnp.logical_and(upper, r == 1),
        jnp.logical_and(upper, r == 3),
    )

    def upper_in(i, cond):
        @pl.when(jnp.logical_and(cond, n + dists[i] < n_seq))
        def _():
            pl.semaphore_wait(ready.at[i], 1)

    def open_forward():
        lax.fori_loop(0, heads, state_body, 0)
        for i in range(3):
            upper_in(i, jnp.logical_not(soon[i]))

        @pl.when(even)
        def _():
            for c in range(heads):
                fsend(0, 1, c, agg.at[c], 1)

    loads[0].wait()
    loads[1].wait()

    upper_in(0, soon[0])

    @pl.when(n == 0)
    def _():
        open_forward()

    def halves(j):
        odd = (tiers + j - 1) % 2
        return odd, 2.0 ** (-((tiers + j - 1 - odd) // 2))

    def reach_level(j, h, g):
        odd, whole = halves(j)
        s = nn(qt[odd, h], mb[j] * g) * whole
        reach[j, h] = s
        out[j, h] = s.astype(BF16)

    go_copy.wait_recv()

    def finish_body(h, carry):
        g = (gacc[:, cols(h)] + nt(gop[...], wv[cols(h), other_cols])).astype(BF16)
        gm[:, cols(h)] = g

        @pl.when(upper)
        def _():
            reach_level(top_level, h, g)

            @pl.when(r == 0)
            def _():
                umsg(0, 0, h, 1).start()

            @pl.when(r == 2)
            def _():
                umsg(0, 1, h, 1).start()

        return carry

    lax.fori_loop(0, heads, finish_body, 0)

    for i in (1, 2):
        upper_in(i, soon[i])

    def joined(c, slots_in):
        tot = reach[top_level, c]
        for slot in slots_in:
            uwait(slot, c)
            tot = tot + ur[slot, c].astype(F32)
        return tot

    @pl.when(jnp.logical_and(upper, r == 1))
    def _():
        for c in range(heads):
            out[top_level, c] = joined(c, (0,)).astype(BF16)
            umsg(0, 0, c, 2).start()

    @pl.when(jnp.logical_and(upper, r == 3))
    def _():
        @pl.when(inner == 3)
        def _():
            for c in range(heads):
                out[top_level, c] = joined(c, (1, 0)).astype(BF16)
                umsg(0, 2, c, 4).start()

        @pl.when(inner == 7)
        def _():
            pl.semaphore_wait(ready.at[3], 1)
            for c in range(heads):
                out[top_level, c] = joined(c, (1, 0, 2)).astype(BF16)
                umsg(0, 3, c, 8).start()

        @pl.when(inner == 11)
        def _():
            for c in range(heads):
                out[top_level, c] = joined(c, (1, 0)).astype(BF16)
                umsg(0, 2, c, 4).start()

        @pl.when(end)
        def _():
            for c in range(heads):
                out[top_level, c] = joined(c, (1, 0, 2, 3)).astype(BF16)
                umsg(1, 3, c, 1).start()
                umsg(0, 3, c, 4).start()

    next_level = top_level - 1

    def next_body(h, carry):
        @pl.when(up[next_level] == 1)
        def _():
            reach_level(next_level, h, gm[:, cols(h)])

            @pl.when(r == 0)
            def _():
                bmsg(next_level, 2, h, -1).start()

            @pl.when(inner == 11)
            def _():
                bmsg(next_level, 1, h, 4).start()

            @pl.when(last)
            def _():
                bmsg(next_level, 3, h, 8).start()

        return carry

    lax.fori_loop(0, heads, next_body, 0)

    def chain_step(j, where, slot, dist):
        @pl.when(jnp.logical_and(up[j] == 1, where))
        def _():
            for c in range(heads):
                bwait(j, 2, c)
                out[j, c] = (reach[j, c] + br[j, 2, c].astype(F32)).astype(BF16)
                bmsg(j, slot, c, dist).start()

    chain_step(next_level, r == 1, 2, -1)
    chain_step(next_level, inner == 10, 0, 3)
    chain_step(next_level, inner == 14, 2, 7)

    def reach_body(h, carry):
        g = gm[:, cols(h)]
        for j in range(next_level):

            @pl.when(up[j] == 1)
            def _():
                reach_level(j, h, g)

        return carry

    lax.fori_loop(0, heads, reach_body, 0)

    @pl.when(n != 0)
    def _():
        open_forward()

    def blend_block(rows, levels):
        t = lax.broadcasted_iota(jnp.int32, (half, half), 0)
        s = lax.broadcasted_iota(jnp.int32, (half, half), 1)
        spread = jnp.bitwise_xor(t, s)

        def column(level):
            return mv[rows, level : level + 1] * tier_scale(level)

        value = jnp.broadcast_to(column(0), (half, half))
        for level in range(1, levels):
            value = jnp.where(spread >= 1 << (level - 1), column(level), value)
        return jnp.where(s <= t, value, 0.0)

    top, low = pl.ds(0, half), pl.ds(half, half)
    blend[0] = blend_block(top, tiers - 1)
    blend[1] = blend_block(low, tiers - 1)
    blend[2] = jnp.broadcast_to(
        mv[low, tiers - 1 : tiers] * tier_scale(tiers - 1), (half, half)
    )

    def forward_step(j):
        for c in range(heads):
            fwait(j, c)

            @pl.when(r == 3)
            def _():
                @pl.when(nxt[j] == 1)
                def _():
                    fsend(j, 0, c, fr.at[j, c], 4)
                    fsend(j, 1, c, fr.at[j, c], 1)

                if j + 1 < span:

                    @pl.when(nxt[j] == 0)
                    def _():
                        tot = state[c] + fr[j, c].astype(F32)
                        state[c] = tot
                        agg[c] = tot.astype(BF16)

                        @pl.when(source_of(j + 1))
                        def _():
                            fsend(j + 1, 0, c, agg.at[c], 4)
                            fsend(j + 1, 1, c, agg.at[c], 1)

            @pl.when(r < 2)
            def _():
                fsend(j, 1, c, fr.at[j, c], 1)

    def when_forward(j, mine):
        @pl.when(jnp.logical_and(up[j] == 1, mine))
        def _():
            forward_step(j)

    def down(level):
        return {0: (0, 1), 1: (1, 2)}.get(level, (1, 4))

    def back_step(j):
        @pl.when(jnp.logical_and(jnp.logical_and(r == 3, after[j] == 1), up[j] == 0))
        def _():
            slot, dist = down(j - 1)
            for c in range(heads):
                tot = jnp.zeros((HD, HD), F32)
                for source in range(4 if j == next_level else 2):
                    bwait(j, source, c)
                    tot = tot + br[j, source, c].astype(F32)
                total[c] = tot
                out[j - 1, c] = (reach[j - 1, c] + tot).astype(BF16)
                bmsg(j - 1, slot, c, dist).start()
            for c in range(heads):
                bmsg(j - 1, slot, c, dist).wait_send()
            for level in range(j - 2, -1, -1):
                slot, dist = down(level)
                for c in range(heads):
                    out[level, c] = (reach[level, c] + total[c]).astype(BF16)
                    bmsg(level, slot, c, dist).start()

    def local_head(h):
        def parts(ref):
            return ref[top, cols(h)], ref[low, cols(h)]

        qa, qb = parts(qv)
        ka, kb = parts(kv)
        va, vb = parts(vv)
        ga, gb = parts(gm)
        paa = (nt(qa, ka) * blend[0]).astype(BF16)
        pba = (nt(qb, ka) * blend[2]).astype(BF16)
        pbb = (nt(qb, kb) * blend[1]).astype(BF16)
        lo[top, cols(h)] = nn(paa, va)
        lo[low, cols(h)] = nn(pba, va) + nn(pbb, vb)
        vl[top, cols(h)] = tn(paa, ga) + tn(pba, gb)
        vl[low, cols(h)] = tn(pbb, gb)
        daa = (nt(ga, va) * blend[0]).astype(BF16)
        dba = (nt(gb, va) * blend[2]).astype(BF16)
        dbb = (nt(gb, vb) * blend[1]).astype(BF16)
        ql[top, cols(h)] = nn(daa, ka)
        ql[low, cols(h)] = nn(dba, ka) + nn(dbb, kb)
        kl[top, cols(h)] = tn(daa, qa) + tn(dba, qb)
        kl[low, cols(h)] = tn(dbb, qb)

    busy = r != 2

    def local_body(i, carry):
        local_head(i)
        return carry

    lax.fori_loop(0, heads, local_body, 0)

    def bsent(cond, level):
        pending.append((cond, lambda: [bmsg(level, 0, c, 0).wait_send() for c in range(heads)]))

    @pl.when(jnp.logical_and(r == 0, up[2] == 1))
    def _():
        for c in range(heads):
            bmsg(2, 2, c, -1).start()

    @pl.when(r == 2)
    def _():
        for c in range(heads):
            bmsg(1, 0, c, 1).start()

    @pl.when(last)
    def _():
        for level, slot, dist in ((2, 1, 4), (1, 1, 2), (0, 0, 1)):
            for c in range(heads):
                bmsg(level, slot, c, dist).start()

    for j in range(top_level):
        early = False
        if 1 <= j < next_level:
            early = jnp.logical_and(jnp.logical_and(r == 3, after[j + 1] == 1), up[j + 1] == 0)
        bsent(jnp.logical_and(up[j] == 1, jnp.logical_not(early)), j)

    chain_step(2, r == 1, 2, -1)
    chain_step(2, r == 2, 0, 3)

    @pl.when(r == 1)
    def _():
        for c in range(heads):
            fwait(0, c)
            agg[c] = (state[c] + fr[0, c].astype(F32)).astype(BF16)
            fsend(1, 0, c, agg.at[c], 2)
            fsend(1, 1, c, agg.at[c], 1)

    def source_of(level):
        return jnp.logical_and(nxt[level] == 1, up[level] == 0)

    @pl.when(r == 3)
    def _():
        first = source_of(2)
        for c in range(heads):
            fwait(0, c)
            state[c] = state[c] + fr[0, c].astype(F32)
        for c in range(heads):
            fwait(1, c)
            tot = state[c] + fr[1, c].astype(F32)
            state[c] = tot
            agg[c] = tot.astype(BF16)

            @pl.when(first)
            def _():
                fsend(2, 0, c, agg.at[c], 4)
                fsend(2, 1, c, agg.at[c], 1)

    for j in (3, 2):
        back_step(j)

    @pl.when(r == 1)
    def _():
        for c in range(heads):
            bwait(1, 0, c)
            bwait(1, 1, c)
            tot = br[1, 0, c].astype(F32) + br[1, 1, c].astype(F32)
            total[c] = tot
            out[0, c] = (reach[0, c] + tot).astype(BF16)
            bmsg(0, 0, c, 1).start()

    when_forward(2, busy)
    for j in range(3, top_level):
        when_forward(j, busy)
    when_forward(top_level, busy)

    @pl.when(r == 2)
    def _():
        for j in range(1, span):

            @pl.when(up[j] == 1)
            def _():
                for c in range(heads):
                    fwait(j, c)

    for j in range(span):

        @pl.when(up[j] == 0)
        def _():
            fr[j] = jnp.zeros(fr.shape[1:], BF16)

    def mix_copy(h):
        return pltpu.make_async_remote_copy(
            src_ref=mix.at[:, cols(h)], dst_ref=mixp.at[:, cols(h)], send_sem=mx_send.at[h],
            recv_sem=mx_recv.at[h], device_id={"head": other}, device_id_type=MESH,
        )

    def far_body(h, carry):
        q = qv[:, cols(h)]
        qs = (q.astype(F32) * ROOT_HALF).astype(BF16)
        g = gm[:, cols(h)]
        mixed = lo[:, cols(h)]
        query = ql[:, cols(h)]
        for j in range(span):
            odd, whole = halves(j)
            mask = mb[j]
            st = fr[j, h]
            mixed = mixed + nn((qs if odd else q) * mask, st) * whole
            query = query + nt(mask * g, st) * tier_scale(tiers + j)
        mix[:, cols(h)] = mixed.astype(BF16)
        gq[:, cols(h)] = query.astype(BF16)
        mix_copy(h).start()
        return carry

    lax.fori_loop(0, heads, far_body, 0)

    stores = [
        pltpu.make_async_copy(src, dst, out_sem.at[i])
        for i, (src, dst) in enumerate(((gq, gq_hbm.at[0]), (gk, gk_hbm.at[0]), (gv, gv_hbm.at[0]), (lay, lay_hbm.at[0])))
    ]
    stores[0].start()

    w_copy.wait_recv()
    for h in range(heads):
        mix_copy(h).wait_recv()

    tile = 256

    def layer_body(i, carry):
        at = pl.multiple_of(i * tile, tile)
        here = pl.ds(pl.multiple_of(core * half_d + at, HD), tile)
        there = pl.ds(at, tile)
        lay[:, there] = (nn(mix[...], wv[:, here]) + nn(mixp[...], wp[:, there])).astype(BF16)
        return carry

    lax.fori_loop(0, half_d // tile, layer_body, 0)
    stores[3].start()

    @pl.when(even)
    def _():
        for c in range(heads):
            bwait(0, 0, c)
            total[c] = br[0, 0, c].astype(F32)

    @pl.when(last)
    def _():
        total[...] = jnp.zeros(total.shape, F32)

    def back_body(h, carry):
        @pl.when(jnp.logical_not(upper))
        def _():
            uwait(3, h)

            @pl.when(jnp.logical_and(r == 3, jnp.logical_not(last)))
            def _():
                umsg(0, 3, h, 4, ur.at[3, h]).start()

            @pl.when(jnp.logical_or(r < 2, jnp.logical_and(r == 3, jnp.logical_not(last))))
            def _():
                umsg(1, 3, h, 1, ur.at[3, h]).start()

            total[h] = total[h] + ur[3, h].astype(F32)

        back = total[h].astype(BF16)
        gk[:, cols(h)] = (kl[:, cols(h)] + nt(vv[:, cols(h)], back)).astype(BF16)
        gv[:, cols(h)] = (vl[:, cols(h)] + nn(kv[:, cols(h)], back)).astype(BF16)
        return carry

    lax.fori_loop(0, heads, back_body, 0)
    stores[1].start()
    stores[2].start()

    fsent(even, 0, 1)
    fsent(r == 1, 1, 0)
    fsent(r == 1, 1, 1)
    for j in range(2, span):
        sends = jnp.logical_and(r == 3, nxt[j] == 1)
        fsent(sends, j, 0)
        fsent(jnp.logical_or(sends, jnp.logical_and(r < 2, up[j] == 1)), j, 1)

    def usent(cond, which):
        pending.append((cond, lambda: [umsg(which, 3, c, 0).wait_send() for c in range(heads)]))

    lower_hop = jnp.logical_and(jnp.logical_not(upper), jnp.logical_and(r == 3, jnp.logical_not(last)))
    usent(jnp.logical_or(upper, lower_hop), 0)
    lower_near = jnp.logical_or(lower_hop, jnp.logical_and(jnp.logical_not(upper), r < 2))
    usent(jnp.logical_or(end, lower_near), 1)
    for cond, wait in pending:

        @pl.when(cond)
        def _():
            wait()

    go_copy.wait_send()
    w_copy.wait_send()
    for h in range(heads):
        mix_copy(h).wait_send()
    for store in stores:
        store.wait()


def on_device(query_in, key_in, value_in, level_mask, out_weight, grad_out):
    n_seq = lax.axis_size("seq")
    _, length, width = query_in.shape
    heads = width // HD
    half_d = grad_out.shape[2]
    span = n_seq.bit_length() - 1
    half = length // 2
    wide = lambda dtype: pltpu.VMEM((length, width), dtype)
    any_spec = pl.BlockSpec(memory_space=pl.ANY)
    dma = lambda *shape: pltpu.SemaphoreType.DMA(shape)
    layer, gq, gk, gv = pl.pallas_call(
        functools.partial(kernel, n_seq, heads, length, half_d),
        out_shape=(
            jax.ShapeDtypeStruct(grad_out.shape, BF16),
            jax.ShapeDtypeStruct(query_in.shape, BF16),
            jax.ShapeDtypeStruct(query_in.shape, BF16),
            jax.ShapeDtypeStruct(query_in.shape, BF16),
        ),
        in_specs=[any_spec] * 6,
        out_specs=(any_spec,) * 4,
        scratch_shapes=[
            wide(BF16), wide(BF16), wide(BF16),
            pltpu.VMEM((HD, length), jnp.int32),
            pltpu.VMEM((length, HD), F32),
            pltpu.VMEM(out_weight.shape, BF16),
            pltpu.VMEM((length, half_d), BF16),
            pltpu.VMEM((length, half_d), BF16),
            pltpu.VMEM((width, half_d), BF16),
            pltpu.VMEM((3, half, half), F32),
            pltpu.VMEM((span, length, HD), BF16),
            wide(F32), wide(BF16),
            pltpu.VMEM((heads, HD, HD), F32),
            pltpu.VMEM((span, heads, HD, HD), BF16),
            pltpu.VMEM((heads, HD, HD), BF16),
            pltpu.VMEM((span, heads, HD, HD), F32),
            pltpu.VMEM((span, heads, HD, HD), BF16),
            pltpu.VMEM((span, 4, heads, HD, HD), BF16),
            pltpu.VMEM((heads, HD, HD), F32),
            wide(F32), wide(F32), wide(F32), wide(F32),
            wide(BF16), wide(BF16),
            pltpu.VMEM((length, half_d), BF16),
            wide(BF16), wide(BF16), wide(BF16),
            pltpu.VMEM((4, heads, HD, HD), BF16),
            pltpu.VMEM((2, heads, HD, length), BF16),
            dma(6), dma(4), dma(2), dma(2), dma(heads), dma(heads),
            dma(span, 2, heads), dma(span, heads), dma(span, heads), dma(span, 4, heads),
            dma(2, heads), dma(4, heads), pltpu.SemaphoreType.REGULAR((4,)),
        ],
        compiler_params=pltpu.CompilerParams(collective_id=0, has_side_effects=True),
        name="log_linear",
    )(query_in, key_in, value_in, jnp.swapaxes(level_mask, 1, 2), out_weight, grad_out)
    return layer, gq, gk, gv


def solution(mesh):
    return jax.shard_map(
        on_device,
        mesh=mesh,
        in_specs=(
            P(("groups", "batch"), "seq", "head"),
            P(("groups", "batch"), "seq", "head"),
            P(("groups", "batch"), "seq", "head"),
            P(("groups", "batch"), "seq", None),
            P("head", None),
            P(("groups", "batch"), "seq", "head"),
        ),
        out_specs=(
            P(("groups", "batch"), "seq", "head"),
            P(("groups", "batch"), "seq", "head"),
            P(("groups", "batch"), "seq", "head"),
            P(("groups", "batch"), "seq", "head"),
        ),
        check_vma=False,
    )
```

```python
import functools

import jax
import jax.numpy as jnp
import numpy as np
from jax import lax
from jax.experimental import pallas as pl
from jax.experimental.pallas import tpu as pltpu
from jax.sharding import PartitionSpec as P

MESH = pl.DeviceIdType.MESH
HD = 128
F32 = jnp.float32
BF16 = jnp.bfloat16
ROOT_HALF = float(np.float32(2.0**-0.5))


def tier_scale(tier):
    return 1.0 if tier == 0 else float(np.float32(2.0 ** (-(tier - 1) / 2.0)))


def nn(a, b):
    return lax.dot_general(a, b, (((1,), (0,)), ((), ())), preferred_element_type=F32)


def nt(a, b):
    return lax.dot_general(a, b, (((1,), (1,)), ((), ())), preferred_element_type=F32)


def tn(a, b):
    return lax.dot_general(a, b, (((0,), (0,)), ((), ())), preferred_element_type=F32)


def kernel(
    n_seq, heads, length, half_d,
    q_hbm, k_hbm, v_hbm, m_hbm, w_hbm, go_hbm,
    lay_hbm, gq_hbm, gk_hbm, gv_hbm,
    qv, kv, vv, mt, mv, wv, go, gop, wp,
    blend, mb, gacc, gm, state, fr, agg, reach, out, br, total,
    lo, ql, kl, vl, mix, mixp, lay, gq, gk, gv, ur, qt,
    in_sem, out_sem, hs_send, hs_recv, mx_send, mx_recv, fs, fr_sem, bs, br_sem, us, ur_sem, ready,
):
    n = lax.axis_index("seq")
    core = lax.axis_index("head")
    other = 1 - core
    span = n_seq.bit_length() - 1
    tiers = length.bit_length()
    half = length // 2
    r = lax.rem(n, 4)
    up = [lax.rem(n >> j, 2) for j in range(span)]
    nxt = [lax.rem((n + 1) >> j, 2) for j in range(span)]
    top_level = span - 1
    n_half = n_seq // 2
    upper = up[top_level] == 1
    inner = lax.rem(n, n_half)
    after = [lax.rem((inner + 1) >> j, 2) for j in range(top_level)]
    last = inner == n_half - 1
    end = n == n_seq - 1
    pending = []
    slots = m_hbm.shape[1]

    barrier = pltpu.get_barrier_semaphore()
    dists = (1, 2, 4)
    third = r == 3
    pl.semaphore_signal(barrier, inc=1, device_id={"head": other}, device_id_type=MESH)
    for d, cond in ((1, n >= 0), (2, r == 1), (3, third), (4, third)):

        @pl.when(jnp.logical_and(cond, n + d < n_seq))
        def _():
            pl.semaphore_signal(barrier, inc=1, device_id={"seq": n + d}, device_id_type=MESH)

    @pl.when(inner == 7)
    def _():
        for d in (7, 8):
            pl.semaphore_signal(barrier, inc=1, device_id={"seq": n + d}, device_id_type=MESH)

    for first in (0, 3):

        @pl.when(n == first)
        def _():
            pl.semaphore_signal(barrier, inc=1, device_id={"seq": n_seq - 1}, device_id_type=MESH)

    loads = [
        pltpu.make_async_copy(src, dst, in_sem.at[i])
        for i, (src, dst) in enumerate(
            ((k_hbm.at[0], kv), (v_hbm.at[0], vv), (go_hbm.at[0], go), (w_hbm, wv),
             (m_hbm.at[0], mt.at[pl.ds(0, slots)]), (q_hbm.at[0], qv))
        )
    ]
    for i in (5, 4, 2, 3, 0, 1):
        loads[i].start()

    one = lambda cond: cond.astype(jnp.int32)
    far_lower = one(jnp.logical_and(r >= 2, n >= 4))
    pl.semaphore_wait(
        barrier, 1 + one(n >= 1) + one(third) + far_lower + one(inner >= 14) + 2 * one(end)
    )

    own_cols = pl.ds(pl.multiple_of(core * half_d, HD), half_d)
    other_cols = pl.ds(pl.multiple_of(other * half_d, HD), half_d)

    def to_core(src, dst, i):
        return pltpu.make_async_remote_copy(
            src_ref=src, dst_ref=dst, send_sem=hs_send.at[i], recv_sem=hs_recv.at[i],
            device_id={"head": other}, device_id_type=MESH,
        )

    go_copy = to_core(go_hbm.at[0], gop, 0)
    w_copy = to_core(w_hbm.at[:, other_cols], wp, 1)
    go_copy.start()
    w_copy.start()
    for i, d in enumerate(dists):

        @pl.when(jnp.logical_and(n >= d, third if d > 1 else n >= 0))
        def _():
            pl.semaphore_signal(ready.at[i], inc=1, device_id={"seq": n - d}, device_id_type=MESH)

    @pl.when(end)
    def _():
        pl.semaphore_signal(ready.at[3], inc=1, device_id={"seq": n - 8}, device_id_type=MESH)

    def cols(h):
        return pl.ds(pl.multiple_of(h * HD, HD), HD)

    loads[5].wait()
    loads[4].wait()
    mt[slots:, :] = jnp.zeros((HD - slots, length), jnp.int32)
    mv[...] = mt[...].astype(F32).T
    for j in range(span):
        mb[j] = jnp.broadcast_to(mv[:, tiers + j : tiers + j + 1], (length, HD)).astype(BF16)

    def turn_body(h, carry):
        q = qv[:, cols(h)].astype(F32)
        qt[0, h] = q.T.astype(BF16)
        qt[1, h] = (q * ROOT_HALF).T.astype(BF16)
        return carry

    lax.fori_loop(0, heads, turn_body, 0)

    def gm_body(i, carry):
        rows = pl.ds(pl.multiple_of(lax.rem(i, 2) * half, half), half)
        wide = heads * HD // 2
        feats = pl.ds(pl.multiple_of(i // 2 * wide, wide), wide)
        gacc[rows, feats] = nt(go[rows, :], wv[feats, own_cols])
        return carry

    loads[2].wait()
    loads[3].wait()
    lax.fori_loop(0, 4, gm_body, 0)

    def fmsg(level, which, c, src, dist):
        return pltpu.make_async_remote_copy(
            src_ref=src, dst_ref=fr.at[level, c], send_sem=fs.at[level, which, c],
            recv_sem=fr_sem.at[level, c], device_id={"seq": n + dist}, device_id_type=MESH,
        )

    def fwait(level, c):
        fmsg(level, 0, c, fr.at[level, c], 0).wait_recv()

    def fsend(level, which, c, src, dist):
        fmsg(level, which, c, src, dist).start()

    def fsent(cond, level, which):
        pending.append(
            (cond, lambda: [fmsg(level, which, c, fr.at[level, c], 0).wait_send() for c in range(heads)])
        )

    def bmsg(level, slot, c, dist):
        return pltpu.make_async_remote_copy(
            src_ref=out.at[level, c], dst_ref=br.at[level, slot, c], send_sem=bs.at[level, c],
            recv_sem=br_sem.at[level, slot, c], device_id={"seq": n - dist}, device_id_type=MESH,
        )

    def bwait(level, slot, c):
        bmsg(level, slot, c, 0).wait_recv()

    def umsg(which, slot, c, dist, src=None):
        return pltpu.make_async_remote_copy(
            src_ref=out.at[top_level, c] if src is None else src, dst_ref=ur.at[slot, c],
            send_sem=us.at[which, c], recv_sem=ur_sem.at[slot, c],
            device_id={"seq": lax.rem(n + dist, n_seq)}, device_id_type=MESH,
        )

    def uwait(slot, c):
        umsg(0, slot, c, 0).wait_recv()

    even = lax.rem(r, 2) == 0

    def state_body(h, carry):
        s = tn(kv[:, cols(h)], vv[:, cols(h)])
        state[h] = s
        agg[h] = s.astype(BF16)
        return carry

    soon = (
        jnp.logical_or(upper, r < 2),
        jnp.logical_and(upper, r == 1),
        jnp.logical_and(upper, r == 3),
    )

    def upper_in(i, cond):
        mine = (n >= 0, r == 1, third)[i]

        @pl.when(jnp.logical_and(jnp.logical_and(cond, mine), n + dists[i] < n_seq))
        def _():
            pl.semaphore_wait(ready.at[i], 1)

    def open_forward():
        lax.fori_loop(0, heads, state_body, 0)
        for i in range(3):
            upper_in(i, jnp.logical_not(soon[i]))

        @pl.when(even)
        def _():
            for c in range(heads):
                fsend(0, 1, c, agg.at[c], 1)

    loads[0].wait()
    loads[1].wait()

    upper_in(0, soon[0])

    @pl.when(n == 0)
    def _():
        open_forward()

    def halves(j):
        odd = (tiers + j - 1) % 2
        return odd, 2.0 ** (-((tiers + j - 1 - odd) // 2))

    def reach_level(j, h, g):
        odd, whole = halves(j)
        s = nn(qt[odd, h], mb[j] * g) * whole
        reach[j, h] = s
        out[j, h] = s.astype(BF16)

    go_copy.wait_recv()

    def finish_body(h, carry):
        g = (gacc[:, cols(h)] + nt(gop[...], wv[cols(h), other_cols])).astype(BF16)
        gm[:, cols(h)] = g

        @pl.when(upper)
        def _():
            reach_level(top_level, h, g)

            @pl.when(r == 0)
            def _():
                umsg(0, 0, h, 1).start()

            @pl.when(r == 2)
            def _():
                umsg(0, 1, h, 1).start()

        return carry

    lax.fori_loop(0, heads, finish_body, 0)

    for i in (1, 2):
        upper_in(i, soon[i])

    def joined(c, slots_in):
        tot = reach[top_level, c]
        for slot in slots_in:
            uwait(slot, c)
            tot = tot + ur[slot, c].astype(F32)
        return tot

    @pl.when(jnp.logical_and(upper, r == 1))
    def _():
        for c in range(heads):
            out[top_level, c] = joined(c, (0,)).astype(BF16)
            umsg(0, 0, c, 2).start()

    @pl.when(jnp.logical_and(upper, r == 3))
    def _():
        @pl.when(inner == 3)
        def _():
            for c in range(heads):
                out[top_level, c] = joined(c, (1, 0)).astype(BF16)
                umsg(0, 2, c, 4).start()

        @pl.when(inner == 7)
        def _():
            pl.semaphore_wait(ready.at[3], 1)
            for c in range(heads):
                out[top_level, c] = joined(c, (1, 0, 2)).astype(BF16)
                umsg(0, 3, c, 8).start()

        @pl.when(inner == 11)
        def _():
            for c in range(heads):
                out[top_level, c] = joined(c, (1, 0)).astype(BF16)
                umsg(0, 2, c, 4).start()

        @pl.when(end)
        def _():
            for c in range(heads):
                out[top_level, c] = joined(c, (1, 0, 2, 3)).astype(BF16)
                umsg(1, 3, c, 1).start()
            for c in range(heads):
                umsg(0, 3, c, 4).start()

    next_level = top_level - 1

    def next_body(h, carry):
        @pl.when(up[next_level] == 1)
        def _():
            reach_level(next_level, h, gm[:, cols(h)])

            @pl.when(r == 0)
            def _():
                bmsg(next_level, 2, h, -1).start()

            @pl.when(inner == 11)
            def _():
                bmsg(next_level, 1, h, 4).start()

            @pl.when(last)
            def _():
                bmsg(next_level, 3, h, 8).start()

        return carry

    lax.fori_loop(0, heads, next_body, 0)

    def chain_step(j, where, slot, dist):
        @pl.when(jnp.logical_and(up[j] == 1, where))
        def _():
            for c in range(heads):
                bwait(j, 2, c)
                out[j, c] = (reach[j, c] + br[j, 2, c].astype(F32)).astype(BF16)
                bmsg(j, slot, c, dist).start()

    chain_step(next_level, r == 1, 2, -1)
    chain_step(next_level, inner == 10, 0, 3)
    chain_step(next_level, inner == 14, 2, 7)

    def reach_body(h, carry):
        g = gm[:, cols(h)]
        for j in range(next_level):

            @pl.when(up[j] == 1)
            def _():
                reach_level(j, h, g)

        return carry

    lax.fori_loop(0, heads, reach_body, 0)

    @pl.when(n != 0)
    def _():
        open_forward()

    def blend_block(rows, levels):
        t = lax.broadcasted_iota(jnp.int32, (half, half), 0)
        s = lax.broadcasted_iota(jnp.int32, (half, half), 1)
        spread = jnp.bitwise_xor(t, s)

        def column(level):
            return mv[rows, level : level + 1] * tier_scale(level)

        value = jnp.broadcast_to(column(0), (half, half))
        for level in range(1, levels):
            value = jnp.where(spread >= 1 << (level - 1), column(level), value)
        return jnp.where(s <= t, value, 0.0)

    top, low = pl.ds(0, half), pl.ds(half, half)
    blend[0] = blend_block(top, tiers - 1)
    blend[1] = blend_block(low, tiers - 1)
    blend[2] = jnp.broadcast_to(
        mv[low, tiers - 1 : tiers] * tier_scale(tiers - 1), (half, half)
    )

    def forward_step(j):
        for c in range(heads):
            fwait(j, c)

            @pl.when(r == 3)
            def _():
                @pl.when(nxt[j] == 1)
                def _():
                    fsend(j, 0, c, fr.at[j, c], 4)
                    fsend(j, 1, c, fr.at[j, c], 1)

                if j + 1 < span:

                    @pl.when(nxt[j] == 0)
                    def _():
                        tot = state[c] + fr[j, c].astype(F32)
                        state[c] = tot
                        agg[c] = tot.astype(BF16)

                        @pl.when(source_of(j + 1))
                        def _():
                            fsend(j + 1, 0, c, agg.at[c], 4)
                            fsend(j + 1, 1, c, agg.at[c], 1)

            @pl.when(r < 2)
            def _():
                fsend(j, 1, c, fr.at[j, c], 1)

    def when_forward(j, mine):
        @pl.when(jnp.logical_and(up[j] == 1, mine))
        def _():
            forward_step(j)

    def down(level):
        return {0: (0, 1), 1: (1, 2)}.get(level, (1, 4))

    def back_step(j):
        @pl.when(jnp.logical_and(jnp.logical_and(r == 3, after[j] == 1), up[j] == 0))
        def _():
            slot, dist = down(j - 1)
            for c in range(heads):
                tot = jnp.zeros((HD, HD), F32)
                for source in range(4 if j == next_level else 2):
                    bwait(j, source, c)
                    tot = tot + br[j, source, c].astype(F32)
                total[c] = tot
                out[j - 1, c] = (reach[j - 1, c] + tot).astype(BF16)
                bmsg(j - 1, slot, c, dist).start()
            for c in range(heads):
                bmsg(j - 1, slot, c, dist).wait_send()
            for level in range(j - 2, -1, -1):
                slot, dist = down(level)
                for c in range(heads):
                    out[level, c] = (reach[level, c] + total[c]).astype(BF16)
                    bmsg(level, slot, c, dist).start()

    def local_head(h):
        def parts(ref):
            return ref[top, cols(h)], ref[low, cols(h)]

        qa, qb = parts(qv)
        ka, kb = parts(kv)
        va, vb = parts(vv)
        ga, gb = parts(gm)
        paa = (nt(qa, ka) * blend[0]).astype(BF16)
        pba = (nt(qb, ka) * blend[2]).astype(BF16)
        pbb = (nt(qb, kb) * blend[1]).astype(BF16)
        lo[top, cols(h)] = nn(paa, va)
        lo[low, cols(h)] = nn(pba, va) + nn(pbb, vb)
        vl[top, cols(h)] = tn(paa, ga) + tn(pba, gb)
        vl[low, cols(h)] = tn(pbb, gb)
        daa = (nt(ga, va) * blend[0]).astype(BF16)
        dba = (nt(gb, va) * blend[2]).astype(BF16)
        dbb = (nt(gb, vb) * blend[1]).astype(BF16)
        ql[top, cols(h)] = nn(daa, ka)
        ql[low, cols(h)] = nn(dba, ka) + nn(dbb, kb)
        kl[top, cols(h)] = tn(daa, qa) + tn(dba, qb)
        kl[low, cols(h)] = tn(dbb, qb)

    busy = r != 2

    def local_body(i, carry):
        local_head(i)
        return carry

    lax.fori_loop(0, heads, local_body, 0)

    def bsent(cond, level):
        pending.append((cond, lambda: [bmsg(level, 0, c, 0).wait_send() for c in range(heads)]))

    @pl.when(jnp.logical_and(r == 0, up[2] == 1))
    def _():
        for c in range(heads):
            bmsg(2, 2, c, -1).start()

    @pl.when(r == 2)
    def _():
        for c in range(heads):
            bmsg(1, 0, c, 1).start()

    @pl.when(last)
    def _():
        for level, slot, dist in ((2, 1, 4), (1, 1, 2), (0, 0, 1)):
            for c in range(heads):
                bmsg(level, slot, c, dist).start()

    for j in range(top_level):
        early = False
        if 1 <= j < next_level:
            early = jnp.logical_and(jnp.logical_and(r == 3, after[j + 1] == 1), up[j + 1] == 0)
        bsent(jnp.logical_and(up[j] == 1, jnp.logical_not(early)), j)

    chain_step(2, r == 1, 2, -1)
    chain_step(2, r == 2, 0, 3)

    @pl.when(r == 1)
    def _():
        for c in range(heads):
            fwait(0, c)
            agg[c] = (state[c] + fr[0, c].astype(F32)).astype(BF16)
            fsend(1, 0, c, agg.at[c], 2)
            fsend(1, 1, c, agg.at[c], 1)

    def source_of(level):
        return jnp.logical_and(nxt[level] == 1, up[level] == 0)

    @pl.when(r == 3)
    def _():
        first = source_of(2)
        for c in range(heads):
            fwait(0, c)
            state[c] = state[c] + fr[0, c].astype(F32)
        for c in range(heads):
            fwait(1, c)
            tot = state[c] + fr[1, c].astype(F32)
            state[c] = tot
            agg[c] = tot.astype(BF16)

            @pl.when(first)
            def _():
                fsend(2, 0, c, agg.at[c], 4)
                fsend(2, 1, c, agg.at[c], 1)

    for j in (3, 2):
        back_step(j)

    @pl.when(r == 1)
    def _():
        for c in range(heads):
            bwait(1, 0, c)
            bwait(1, 1, c)
            tot = br[1, 0, c].astype(F32) + br[1, 1, c].astype(F32)
            total[c] = tot
            out[0, c] = (reach[0, c] + tot).astype(BF16)
            bmsg(0, 0, c, 1).start()

    when_forward(2, busy)
    for j in range(3, top_level):
        when_forward(j, busy)
    when_forward(top_level, busy)

    @pl.when(r == 2)
    def _():
        for j in range(1, span):

            @pl.when(up[j] == 1)
            def _():
                for c in range(heads):
                    fwait(j, c)

    for j in range(span):

        @pl.when(up[j] == 0)
        def _():
            fr[j] = jnp.zeros(fr.shape[1:], BF16)

    def mix_copy(h):
        return pltpu.make_async_remote_copy(
            src_ref=mix.at[:, cols(h)], dst_ref=mixp.at[:, cols(h)], send_sem=mx_send.at[h],
            recv_sem=mx_recv.at[h], device_id={"head": other}, device_id_type=MESH,
        )

    def far_body(h, carry):
        q = qv[:, cols(h)]
        qs = (q.astype(F32) * ROOT_HALF).astype(BF16)
        g = gm[:, cols(h)]
        mixed = lo[:, cols(h)]
        query = ql[:, cols(h)]
        for j in range(span):
            odd, whole = halves(j)
            mask = mb[j]
            st = fr[j, h]
            mixed = mixed + nn((qs if odd else q) * mask, st) * whole
            query = query + nt(mask * g, st) * tier_scale(tiers + j)
        mix[:, cols(h)] = mixed.astype(BF16)
        gq[:, cols(h)] = query.astype(BF16)
        mix_copy(h).start()
        return carry

    lax.fori_loop(0, heads, far_body, 0)

    stores = [
        pltpu.make_async_copy(src, dst, out_sem.at[i])
        for i, (src, dst) in enumerate(((gq, gq_hbm.at[0]), (gk, gk_hbm.at[0]), (gv, gv_hbm.at[0]), (lay, lay_hbm.at[0])))
    ]
    stores[0].start()

    w_copy.wait_recv()
    for h in range(heads):
        mix_copy(h).wait_recv()

    tile = 256

    def layer_body(i, carry):
        at = pl.multiple_of(i * tile, tile)
        here = pl.ds(pl.multiple_of(core * half_d + at, HD), tile)
        there = pl.ds(at, tile)
        lay[:, there] = (nn(mix[...], wv[:, here]) + nn(mixp[...], wp[:, there])).astype(BF16)
        return carry

    lax.fori_loop(0, half_d // tile, layer_body, 0)
    stores[3].start()

    @pl.when(even)
    def _():
        for c in range(heads):
            bwait(0, 0, c)
            total[c] = br[0, 0, c].astype(F32)

    @pl.when(last)
    def _():
        total[...] = jnp.zeros(total.shape, F32)

    def back_body(h, carry):
        @pl.when(jnp.logical_not(upper))
        def _():
            uwait(3, h)

            @pl.when(jnp.logical_and(r == 3, jnp.logical_not(last)))
            def _():
                umsg(0, 3, h, 4, ur.at[3, h]).start()

            @pl.when(jnp.logical_or(r < 2, jnp.logical_and(r == 3, jnp.logical_not(last))))
            def _():
                umsg(1, 3, h, 1, ur.at[3, h]).start()

            total[h] = total[h] + ur[3, h].astype(F32)

        back = total[h].astype(BF16)
        gk[:, cols(h)] = (kl[:, cols(h)] + nt(vv[:, cols(h)], back)).astype(BF16)
        gv[:, cols(h)] = (vl[:, cols(h)] + nn(kv[:, cols(h)], back)).astype(BF16)
        return carry

    lax.fori_loop(0, heads, back_body, 0)
    stores[1].start()
    stores[2].start()

    fsent(even, 0, 1)
    fsent(r == 1, 1, 0)
    fsent(r == 1, 1, 1)
    for j in range(2, span):
        sends = jnp.logical_and(r == 3, nxt[j] == 1)
        fsent(sends, j, 0)
        fsent(jnp.logical_or(sends, jnp.logical_and(r < 2, up[j] == 1)), j, 1)

    def usent(cond, which):
        pending.append((cond, lambda: [umsg(which, 3, c, 0).wait_send() for c in range(heads)]))

    lower_hop = jnp.logical_and(jnp.logical_not(upper), jnp.logical_and(r == 3, jnp.logical_not(last)))
    usent(jnp.logical_or(upper, lower_hop), 0)
    lower_near = jnp.logical_or(lower_hop, jnp.logical_and(jnp.logical_not(upper), r < 2))
    usent(jnp.logical_or(end, lower_near), 1)
    for cond, wait in pending:

        @pl.when(cond)
        def _():
            wait()

    go_copy.wait_send()
    w_copy.wait_send()
    for h in range(heads):
        mix_copy(h).wait_send()
    for store in stores:
        store.wait()


def settle(pieces, *refs):
    sources, outs, went = refs[:4], refs[4:8], refs[8]
    copies = [
        pltpu.make_async_copy(
            sources[which].at[0, pl.ds(at, rows)], outs[which].at[0, pl.ds(at, rows)], went.at[i]
        )
        for i, (which, at, rows) in enumerate(pieces)
    ]
    for copy in copies:
        copy.start()
    for copy in copies:
        copy.wait()


def on_device(query_in, key_in, value_in, level_mask, out_weight, grad_out):
    n_seq = lax.axis_size("seq")
    _, length, width = query_in.shape
    heads = width // HD
    half_d = grad_out.shape[2]
    span = n_seq.bit_length() - 1
    half = length // 2
    wide = lambda dtype: pltpu.VMEM((length, width), dtype)
    any_spec = pl.BlockSpec(memory_space=pl.ANY)
    dma = lambda *shape: pltpu.SemaphoreType.DMA(shape)
    layer, gq, gk, gv = pl.pallas_call(
        functools.partial(kernel, n_seq, heads, length, half_d),
        out_shape=(
            jax.ShapeDtypeStruct(grad_out.shape, BF16),
            jax.ShapeDtypeStruct(query_in.shape, BF16),
            jax.ShapeDtypeStruct(query_in.shape, BF16),
            jax.ShapeDtypeStruct(query_in.shape, BF16),
        ),
        in_specs=[pl.BlockSpec(memory_space=pltpu.HBM)] * 6,
        out_specs=(any_spec,) * 4,
        scratch_shapes=[
            wide(BF16), wide(BF16), wide(BF16),
            pltpu.VMEM((HD, length), jnp.int32),
            pltpu.VMEM((length, HD), F32),
            pltpu.VMEM(out_weight.shape, BF16),
            pltpu.VMEM((length, half_d), BF16),
            pltpu.VMEM((length, half_d), BF16),
            pltpu.VMEM((width, half_d), BF16),
            pltpu.VMEM((3, half, half), F32),
            pltpu.VMEM((span, length, HD), BF16),
            wide(F32), wide(BF16),
            pltpu.VMEM((heads, HD, HD), F32),
            pltpu.VMEM((span, heads, HD, HD), BF16),
            pltpu.VMEM((heads, HD, HD), BF16),
            pltpu.VMEM((span, heads, HD, HD), F32),
            pltpu.VMEM((span, heads, HD, HD), BF16),
            pltpu.VMEM((span, 4, heads, HD, HD), BF16),
            pltpu.VMEM((heads, HD, HD), F32),
            wide(F32), wide(F32), wide(F32), wide(F32),
            wide(BF16), wide(BF16),
            pltpu.VMEM((length, half_d), BF16),
            wide(BF16), wide(BF16), wide(BF16),
            pltpu.VMEM((4, heads, HD, HD), BF16),
            pltpu.VMEM((2, heads, HD, length), BF16),
            dma(6), dma(4), dma(2), dma(2), dma(heads), dma(heads),
            dma(span, 2, heads), dma(span, heads), dma(span, heads), dma(span, 4, heads),
            dma(2, heads), dma(4, heads), pltpu.SemaphoreType.REGULAR((4,)),
        ],
        compiler_params=pltpu.CompilerParams(collective_id=0, has_side_effects=True, vmem_limit_bytes=57 << 20),
        name="log_linear",
    )(query_in, key_in, value_in, jnp.swapaxes(level_mask, 1, 2), out_weight, grad_out)
    results = (layer, gq, gk, gv)
    pieces = [(0, i * length // 4, length // 4) for i in range(4)]
    pieces += [(which, i * half, half) for which in (1, 2, 3) for i in range(2)]
    return pl.pallas_call(
        functools.partial(settle, pieces),
        out_shape=tuple(jax.ShapeDtypeStruct(x.shape, x.dtype) for x in results),
        in_specs=[any_spec] * 4,
        out_specs=(any_spec,) * 4,
        scratch_shapes=[dma(len(pieces))],
        compiler_params=pltpu.CompilerParams(vmem_limit_bytes=8 << 20),
        name="settle",
    )(*results)


def solution(mesh):
    return jax.shard_map(
        on_device,
        mesh=mesh,
        in_specs=(
            P(("groups", "batch"), "seq", "head"),
            P(("groups", "batch"), "seq", "head"),
            P(("groups", "batch"), "seq", "head"),
            P(("groups", "batch"), "seq", None),
            P("head", None),
            P(("groups", "batch"), "seq", "head"),
        ),
        out_specs=(
            P(("groups", "batch"), "seq", "head"),
            P(("groups", "batch"), "seq", "head"),
            P(("groups", "batch"), "seq", "head"),
            P(("groups", "batch"), "seq", "head"),
        ),
        check_vma=False,
    )
```

```python
import functools

import jax
import jax.numpy as jnp
import numpy as np
from jax import lax
from jax.experimental import pallas as pl
from jax.experimental.pallas import tpu as pltpu
from jax.sharding import PartitionSpec as P

MESH = pl.DeviceIdType.MESH
HD = 128
F32 = jnp.float32
BF16 = jnp.bfloat16
ROOT_HALF = float(np.float32(2.0**-0.5))


def tier_scale(tier):
    return 1.0 if tier == 0 else float(np.float32(2.0 ** (-(tier - 1) / 2.0)))


def nn(a, b):
    return lax.dot_general(a, b, (((1,), (0,)), ((), ())), preferred_element_type=F32)


def nt(a, b):
    return lax.dot_general(a, b, (((1,), (1,)), ((), ())), preferred_element_type=F32)


def tn(a, b):
    return lax.dot_general(a, b, (((0,), (0,)), ((), ())), preferred_element_type=F32)


def kernel(
    n_seq, heads, length, half_d,
    q_hbm, k_hbm, v_hbm, m_hbm, w_hbm, go_hbm,
    lay_hbm, gq_hbm, gk_hbm, gv_hbm,
    qv, kv, vv, mt, mv, wv, go, gop, wp,
    blend, mb, gacc, gm, state, fr, agg, reach, out, br, total,
    lo, ql, kl, vl, mix, mixp, lay, gq, gk, gv, ur, qt,
    in_sem, out_sem, hs_send, hs_recv, mx_send, mx_recv, fs, fr_sem, bs, br_sem, us, ur_sem, ready,
):
    n = lax.axis_index("seq")
    core = lax.axis_index("head")
    other = 1 - core
    span = n_seq.bit_length() - 1
    tiers = length.bit_length()
    half = length // 2
    r = lax.rem(n, 4)
    up = [lax.rem(n >> j, 2) for j in range(span)]
    nxt = [lax.rem((n + 1) >> j, 2) for j in range(span)]
    top_level = span - 1
    n_half = n_seq // 2
    upper = up[top_level] == 1
    inner = lax.rem(n, n_half)
    after = [lax.rem((inner + 1) >> j, 2) for j in range(top_level)]
    last = inner == n_half - 1
    end = n == n_seq - 1
    pending = []
    slots = m_hbm.shape[1]

    barrier = pltpu.get_barrier_semaphore()
    dists = (1, 2, 4)
    third = r == 3
    pl.semaphore_signal(barrier, inc=1, device_id={"head": other}, device_id_type=MESH)
    for d, cond in ((1, n >= 0), (2, r == 1), (3, third), (4, third)):

        @pl.when(jnp.logical_and(cond, n + d < n_seq))
        def _():
            pl.semaphore_signal(barrier, inc=1, device_id={"seq": n + d}, device_id_type=MESH)

    @pl.when(inner == 7)
    def _():
        for d in (7, 8):
            pl.semaphore_signal(barrier, inc=1, device_id={"seq": n + d}, device_id_type=MESH)

    for first in (0, 3):

        @pl.when(n == first)
        def _():
            pl.semaphore_signal(barrier, inc=1, device_id={"seq": n_seq - 1}, device_id_type=MESH)

    loads = [
        pltpu.make_async_copy(src, dst, in_sem.at[i])
        for i, (src, dst) in enumerate(
            ((k_hbm.at[0], kv), (v_hbm.at[0], vv), (go_hbm.at[0], go), (w_hbm, wv),
             (m_hbm.at[0], mt.at[pl.ds(0, slots)]), (q_hbm.at[0], qv))
        )
    ]
    for i in (5, 4, 2, 3, 0, 1):
        loads[i].start()

    one = lambda cond: cond.astype(jnp.int32)
    far_lower = one(jnp.logical_and(r >= 2, n >= 4))
    pl.semaphore_wait(
        barrier, 1 + one(n >= 1) + one(third) + far_lower + one(inner >= 14) + 2 * one(end)
    )

    own_cols = pl.ds(pl.multiple_of(core * half_d, HD), half_d)
    other_cols = pl.ds(pl.multiple_of(other * half_d, HD), half_d)

    def to_core(src, dst, i):
        return pltpu.make_async_remote_copy(
            src_ref=src, dst_ref=dst, send_sem=hs_send.at[i], recv_sem=hs_recv.at[i],
            device_id={"head": other}, device_id_type=MESH,
        )

    go_copy = to_core(go_hbm.at[0], gop, 0)
    w_copy = to_core(w_hbm.at[:, other_cols], wp, 1)
    go_copy.start()
    w_copy.start()
    for i, d in enumerate(dists):

        @pl.when(jnp.logical_and(n >= d, third if d > 1 else n >= 0))
        def _():
            pl.semaphore_signal(ready.at[i], inc=1, device_id={"seq": n - d}, device_id_type=MESH)

    @pl.when(end)
    def _():
        pl.semaphore_signal(ready.at[3], inc=1, device_id={"seq": n - 8}, device_id_type=MESH)

    def cols(h):
        return pl.ds(pl.multiple_of(h * HD, HD), HD)

    loads[5].wait()
    loads[4].wait()
    mt[slots:, :] = jnp.zeros((HD - slots, length), jnp.int32)
    mv[...] = mt[...].astype(F32).T
    for j in range(span):
        mb[j] = jnp.broadcast_to(mv[:, tiers + j : tiers + j + 1], (length, HD)).astype(BF16)

    def turn_body(h, carry):
        q = qv[:, cols(h)].astype(F32)
        qt[0, h] = q.T.astype(BF16)
        qt[1, h] = (q * ROOT_HALF).T.astype(BF16)
        return carry

    lax.fori_loop(0, heads, turn_body, 0)

    def gm_body(i, carry):
        rows = pl.ds(pl.multiple_of(lax.rem(i, 2) * half, half), half)
        wide = heads * HD // 2
        feats = pl.ds(pl.multiple_of(i // 2 * wide, wide), wide)
        gacc[rows, feats] = nt(go[rows, :], wv[feats, own_cols])
        return carry

    loads[2].wait()
    loads[3].wait()
    lax.fori_loop(0, 4, gm_body, 0)

    def fmsg(level, which, c, src, dist):
        return pltpu.make_async_remote_copy(
            src_ref=src, dst_ref=fr.at[level, c], send_sem=fs.at[level, which, c],
            recv_sem=fr_sem.at[level, c], device_id={"seq": n + dist}, device_id_type=MESH,
        )

    def fwait(level, c):
        fmsg(level, 0, c, fr.at[level, c], 0).wait_recv()

    def fsend(level, which, c, src, dist):
        fmsg(level, which, c, src, dist).start()

    def fsent(cond, level, which):
        pending.append(
            (cond, lambda: [fmsg(level, which, c, fr.at[level, c], 0).wait_send() for c in range(heads)])
        )

    def bmsg(level, slot, c, dist):
        return pltpu.make_async_remote_copy(
            src_ref=out.at[level, c], dst_ref=br.at[level, slot, c], send_sem=bs.at[level, c],
            recv_sem=br_sem.at[level, slot, c], device_id={"seq": n - dist}, device_id_type=MESH,
        )

    def bwait(level, slot, c):
        bmsg(level, slot, c, 0).wait_recv()

    def umsg(which, slot, c, dist, src=None):
        return pltpu.make_async_remote_copy(
            src_ref=out.at[top_level, c] if src is None else src, dst_ref=ur.at[slot, c],
            send_sem=us.at[which, c], recv_sem=ur_sem.at[slot, c],
            device_id={"seq": lax.rem(n + dist, n_seq)}, device_id_type=MESH,
        )

    def uwait(slot, c):
        umsg(0, slot, c, 0).wait_recv()

    even = lax.rem(r, 2) == 0

    def state_body(h, carry):
        s = tn(kv[:, cols(h)], vv[:, cols(h)])
        state[h] = s
        agg[h] = s.astype(BF16)
        return carry

    soon = (
        jnp.logical_or(upper, r < 2),
        jnp.logical_and(upper, r == 1),
        jnp.logical_and(upper, r == 3),
    )

    def upper_in(i, cond):
        mine = (n >= 0, r == 1, third)[i]

        @pl.when(jnp.logical_and(jnp.logical_and(cond, mine), n + dists[i] < n_seq))
        def _():
            pl.semaphore_wait(ready.at[i], 1)

    def open_forward():
        lax.fori_loop(0, heads, state_body, 0)
        for i in range(3):
            upper_in(i, jnp.logical_not(soon[i]))

        @pl.when(even)
        def _():
            for c in range(heads):
                fsend(0, 1, c, agg.at[c], 1)

    loads[0].wait()
    loads[1].wait()

    upper_in(0, soon[0])

    @pl.when(n == 0)
    def _():
        open_forward()

    def halves(j):
        odd = (tiers + j - 1) % 2
        return odd, 2.0 ** (-((tiers + j - 1 - odd) // 2))

    def reach_level(j, h, g):
        odd, whole = halves(j)
        s = nn(qt[odd, h], mb[j] * g) * whole
        reach[j, h] = s
        out[j, h] = s.astype(BF16)

    go_copy.wait_recv()

    def finish_body(h, carry):
        g = (gacc[:, cols(h)] + nt(gop[...], wv[cols(h), other_cols])).astype(BF16)
        gm[:, cols(h)] = g

        @pl.when(upper)
        def _():
            reach_level(top_level, h, g)

            @pl.when(r == 0)
            def _():
                umsg(0, 0, h, 1).start()

            @pl.when(r == 2)
            def _():
                umsg(0, 1, h, 1).start()

        return carry

    lax.fori_loop(0, heads, finish_body, 0)

    for i in (1, 2):
        upper_in(i, soon[i])

    def joined(c, slots_in):
        tot = reach[top_level, c]
        for slot in slots_in:
            uwait(slot, c)
            tot = tot + ur[slot, c].astype(F32)
        return tot

    @pl.when(jnp.logical_and(upper, r == 1))
    def _():
        for c in range(heads):
            out[top_level, c] = joined(c, (0,)).astype(BF16)
            umsg(0, 0, c, 2).start()

    @pl.when(jnp.logical_and(upper, r == 3))
    def _():
        @pl.when(inner == 3)
        def _():
            for c in range(heads):
                out[top_level, c] = joined(c, (1, 0)).astype(BF16)
                umsg(0, 2, c, 4).start()

        @pl.when(inner == 7)
        def _():
            pl.semaphore_wait(ready.at[3], 1)
            for c in range(heads):
                out[top_level, c] = joined(c, (1, 0, 2)).astype(BF16)
                umsg(0, 3, c, 8).start()

        @pl.when(inner == 11)
        def _():
            for c in range(heads):
                out[top_level, c] = joined(c, (1, 0)).astype(BF16)
                umsg(0, 2, c, 4).start()

        @pl.when(end)
        def _():
            for c in range(heads):
                out[top_level, c] = joined(c, (1, 0, 2, 3)).astype(BF16)
                umsg(1, 3, c, 1).start()
            for c in range(heads):
                umsg(0, 3, c, 4).start()

    next_level = top_level - 1

    def next_body(h, carry):
        @pl.when(up[next_level] == 1)
        def _():
            reach_level(next_level, h, gm[:, cols(h)])

            @pl.when(r == 0)
            def _():
                bmsg(next_level, 2, h, -1).start()

            @pl.when(inner == 11)
            def _():
                bmsg(next_level, 1, h, 4).start()

            @pl.when(last)
            def _():
                bmsg(next_level, 3, h, 8).start()

        return carry

    lax.fori_loop(0, heads, next_body, 0)

    def chain_step(j, where, slot, dist):
        @pl.when(jnp.logical_and(up[j] == 1, where))
        def _():
            for c in range(heads):
                bwait(j, 2, c)
                out[j, c] = (reach[j, c] + br[j, 2, c].astype(F32)).astype(BF16)
                bmsg(j, slot, c, dist).start()

    chain_step(next_level, r == 1, 2, -1)
    chain_step(next_level, inner == 10, 0, 3)
    chain_step(next_level, inner == 14, 2, 7)

    def reach_body(h, carry):
        g = gm[:, cols(h)]
        for j in range(next_level):

            @pl.when(up[j] == 1)
            def _():
                reach_level(j, h, g)

        return carry

    lax.fori_loop(0, heads, reach_body, 0)

    @pl.when(n != 0)
    def _():
        open_forward()

    def blend_block(rows, levels):
        t = lax.broadcasted_iota(jnp.int32, (half, half), 0)
        s = lax.broadcasted_iota(jnp.int32, (half, half), 1)
        spread = jnp.bitwise_xor(t, s)

        def column(level):
            return mv[rows, level : level + 1] * tier_scale(level)

        value = jnp.broadcast_to(column(0), (half, half))
        for level in range(1, levels):
            value = jnp.where(spread >= 1 << (level - 1), column(level), value)
        return jnp.where(s <= t, value, 0.0)

    top, low = pl.ds(0, half), pl.ds(half, half)
    blend[0] = blend_block(top, tiers - 1)
    blend[1] = blend_block(low, tiers - 1)
    blend[2] = jnp.broadcast_to(
        mv[low, tiers - 1 : tiers] * tier_scale(tiers - 1), (half, half)
    )

    def forward_step(j):
        for c in range(heads):
            fwait(j, c)

            @pl.when(r == 3)
            def _():
                @pl.when(nxt[j] == 1)
                def _():
                    fsend(j, 0, c, fr.at[j, c], 4)
                    fsend(j, 1, c, fr.at[j, c], 1)

                if j + 1 < span:

                    @pl.when(nxt[j] == 0)
                    def _():
                        tot = state[c] + fr[j, c].astype(F32)
                        state[c] = tot
                        agg[c] = tot.astype(BF16)

                        @pl.when(source_of(j + 1))
                        def _():
                            fsend(j + 1, 0, c, agg.at[c], 4)
                            fsend(j + 1, 1, c, agg.at[c], 1)

            @pl.when(r < 2)
            def _():
                fsend(j, 1, c, fr.at[j, c], 1)

    def when_forward(j, mine):
        @pl.when(jnp.logical_and(up[j] == 1, mine))
        def _():
            forward_step(j)

    def down(level):
        return {0: (0, 1), 1: (1, 2)}.get(level, (1, 4))

    def back_step(j, where):
        @pl.when(jnp.logical_and(jnp.logical_and(where, after[j] == 1), up[j] == 0))
        def _():
            slot, dist = down(j - 1)
            for c in range(heads):
                tot = jnp.zeros((HD, HD), F32)
                for source in range(4 if j == next_level else 2):
                    bwait(j, source, c)
                    tot = tot + br[j, source, c].astype(F32)
                total[c] = tot
                out[j - 1, c] = (reach[j - 1, c] + tot).astype(BF16)
                bmsg(j - 1, slot, c, dist).start()
            for c in range(heads):
                bmsg(j - 1, slot, c, dist).wait_send()
            for level in range(j - 2, -1, -1):
                slot, dist = down(level)
                for c in range(heads):
                    out[level, c] = (reach[level, c] + total[c]).astype(BF16)
                    bmsg(level, slot, c, dist).start()

    def local_head(h):
        def parts(ref):
            return ref[top, cols(h)], ref[low, cols(h)]

        qa, qb = parts(qv)
        ka, kb = parts(kv)
        va, vb = parts(vv)
        ga, gb = parts(gm)
        paa = (nt(qa, ka) * blend[0]).astype(BF16)
        pba = (nt(qb, ka) * blend[2]).astype(BF16)
        pbb = (nt(qb, kb) * blend[1]).astype(BF16)
        lo[top, cols(h)] = nn(paa, va)
        lo[low, cols(h)] = nn(pba, va) + nn(pbb, vb)
        vl[top, cols(h)] = tn(paa, ga) + tn(pba, gb)
        vl[low, cols(h)] = tn(pbb, gb)
        daa = (nt(ga, va) * blend[0]).astype(BF16)
        dba = (nt(gb, va) * blend[2]).astype(BF16)
        dbb = (nt(gb, vb) * blend[1]).astype(BF16)
        ql[top, cols(h)] = nn(daa, ka)
        ql[low, cols(h)] = nn(dba, ka) + nn(dbb, kb)
        kl[top, cols(h)] = tn(daa, qa) + tn(dba, qb)
        kl[low, cols(h)] = tn(dbb, qb)

    busy = r != 2

    def local_body(i, carry):
        local_head(i)
        return carry

    @pl.when(r == 1)
    def _():
        for c in range(heads):
            fwait(0, c)
            agg[c] = (state[c] + fr[0, c].astype(F32)).astype(BF16)
            fsend(1, 0, c, agg.at[c], 2)
        for c in range(heads):
            fsend(1, 1, c, agg.at[c], 1)

    lax.fori_loop(0, heads, local_body, 0)

    def bsent(cond, level):
        pending.append((cond, lambda: [bmsg(level, 0, c, 0).wait_send() for c in range(heads)]))

    @pl.when(jnp.logical_and(r == 0, up[2] == 1))
    def _():
        for c in range(heads):
            bmsg(2, 2, c, -1).start()

    @pl.when(r == 2)
    def _():
        for c in range(heads):
            bmsg(1, 0, c, 1).start()

    @pl.when(last)
    def _():
        for level, slot, dist in ((2, 1, 4), (1, 1, 2), (0, 0, 1)):
            for c in range(heads):
                bmsg(level, slot, c, dist).start()

    for j in range(top_level):
        early = False
        if 1 <= j < next_level:
            early = jnp.logical_and(jnp.logical_and(r == 3, after[j + 1] == 1), up[j + 1] == 0)
        bsent(jnp.logical_and(up[j] == 1, jnp.logical_not(early)), j)

    chain_step(2, r == 1, 2, -1)
    chain_step(2, r == 2, 0, 3)

    def source_of(level):
        return jnp.logical_and(nxt[level] == 1, up[level] == 0)

    back_step(2, n == 3)

    @pl.when(r == 3)
    def _():
        first = source_of(2)
        for c in range(heads):
            fwait(0, c)
            state[c] = state[c] + fr[0, c].astype(F32)
        for c in range(heads):
            fwait(1, c)
            tot = state[c] + fr[1, c].astype(F32)
            state[c] = tot
            agg[c] = tot.astype(BF16)

            @pl.when(first)
            def _():
                fsend(2, 0, c, agg.at[c], 4)
                fsend(2, 1, c, agg.at[c], 1)

    for j in (3, 2):
        back_step(j, jnp.logical_and(r == 3, n != 3))

    @pl.when(r == 1)
    def _():
        for c in range(heads):
            bwait(1, 0, c)
            bwait(1, 1, c)
            tot = br[1, 0, c].astype(F32) + br[1, 1, c].astype(F32)
            total[c] = tot
            out[0, c] = (reach[0, c] + tot).astype(BF16)
            bmsg(0, 0, c, 1).start()

    when_forward(2, busy)
    for j in range(3, top_level):
        when_forward(j, busy)
    when_forward(top_level, busy)

    @pl.when(r == 2)
    def _():
        for j in range(1, span):

            @pl.when(up[j] == 1)
            def _():
                for c in range(heads):
                    fwait(j, c)

    for j in range(span):

        @pl.when(up[j] == 0)
        def _():
            fr[j] = jnp.zeros(fr.shape[1:], BF16)

    def mix_copy(h):
        return pltpu.make_async_remote_copy(
            src_ref=mix.at[:, cols(h)], dst_ref=mixp.at[:, cols(h)], send_sem=mx_send.at[h],
            recv_sem=mx_recv.at[h], device_id={"head": other}, device_id_type=MESH,
        )

    def far_body(h, carry):
        q = qv[:, cols(h)]
        qs = (q.astype(F32) * ROOT_HALF).astype(BF16)
        g = gm[:, cols(h)]
        mixed = lo[:, cols(h)]
        query = ql[:, cols(h)]
        for j in range(span):
            odd, whole = halves(j)
            mask = mb[j]
            st = fr[j, h]
            mixed = mixed + nn((qs if odd else q) * mask, st) * whole
            query = query + nt(mask * g, st) * tier_scale(tiers + j)
        mix[:, cols(h)] = mixed.astype(BF16)
        gq[:, cols(h)] = query.astype(BF16)
        mix_copy(h).start()
        return carry

    lax.fori_loop(0, heads, far_body, 0)

    stores = [
        pltpu.make_async_copy(src, dst, out_sem.at[i])
        for i, (src, dst) in enumerate(((gq, gq_hbm.at[0]), (gk, gk_hbm.at[0]), (gv, gv_hbm.at[0]), (lay, lay_hbm.at[0])))
    ]
    stores[0].start()

    w_copy.wait_recv()
    for h in range(heads):
        mix_copy(h).wait_recv()

    tile = 256

    def layer_body(i, carry):
        at = pl.multiple_of(i * tile, tile)
        here = pl.ds(pl.multiple_of(core * half_d + at, HD), tile)
        there = pl.ds(at, tile)
        lay[:, there] = (nn(mix[...], wv[:, here]) + nn(mixp[...], wp[:, there])).astype(BF16)
        return carry

    lax.fori_loop(0, half_d // tile, layer_body, 0)
    stores[3].start()

    @pl.when(even)
    def _():
        for c in range(heads):
            bwait(0, 0, c)
            total[c] = br[0, 0, c].astype(F32)

    @pl.when(last)
    def _():
        total[...] = jnp.zeros(total.shape, F32)

    def back_body(h, carry):
        @pl.when(jnp.logical_not(upper))
        def _():
            uwait(3, h)

            @pl.when(jnp.logical_and(r == 3, jnp.logical_not(last)))
            def _():
                umsg(0, 3, h, 4, ur.at[3, h]).start()

            @pl.when(jnp.logical_or(r < 2, jnp.logical_and(r == 3, jnp.logical_not(last))))
            def _():
                umsg(1, 3, h, 1, ur.at[3, h]).start()

            total[h] = total[h] + ur[3, h].astype(F32)

        back = total[h].astype(BF16)
        gk[:, cols(h)] = (kl[:, cols(h)] + nt(vv[:, cols(h)], back)).astype(BF16)
        gv[:, cols(h)] = (vl[:, cols(h)] + nn(kv[:, cols(h)], back)).astype(BF16)
        return carry

    lax.fori_loop(0, heads, back_body, 0)
    stores[1].start()
    stores[2].start()

    fsent(even, 0, 1)
    fsent(r == 1, 1, 0)
    fsent(r == 1, 1, 1)
    for j in range(2, span):
        sends = jnp.logical_and(r == 3, nxt[j] == 1)
        fsent(sends, j, 0)
        fsent(jnp.logical_or(sends, jnp.logical_and(r < 2, up[j] == 1)), j, 1)

    def usent(cond, which):
        pending.append((cond, lambda: [umsg(which, 3, c, 0).wait_send() for c in range(heads)]))

    lower_hop = jnp.logical_and(jnp.logical_not(upper), jnp.logical_and(r == 3, jnp.logical_not(last)))
    usent(jnp.logical_or(upper, lower_hop), 0)
    lower_near = jnp.logical_or(lower_hop, jnp.logical_and(jnp.logical_not(upper), r < 2))
    usent(jnp.logical_or(end, lower_near), 1)
    for cond, wait in pending:

        @pl.when(cond)
        def _():
            wait()

    go_copy.wait_send()
    w_copy.wait_send()
    for h in range(heads):
        mix_copy(h).wait_send()
    for store in stores:
        store.wait()


def settle(pieces, *refs):
    sources, outs, held = refs[:4], refs[4:8], refs[8:12]
    came, went = refs[12], refs[13]
    into, back = [], []
    for i, (which, at, rows) in enumerate(pieces):
        here = pl.ds(at, rows)
        into.append(pltpu.make_async_copy(sources[which].at[0, here], held[which].at[here], came.at[i]))
        back.append(pltpu.make_async_copy(held[which].at[here], outs[which].at[0, here], went.at[i]))
        into[-1].start()
    for i in range(len(pieces)):
        into[i].wait()
        back[i].start()
    for i in range(len(pieces)):
        back[i].wait()


def on_device(query_in, key_in, value_in, level_mask, out_weight, grad_out):
    n_seq = lax.axis_size("seq")
    _, length, width = query_in.shape
    heads = width // HD
    half_d = grad_out.shape[2]
    span = n_seq.bit_length() - 1
    half = length // 2
    wide = lambda dtype: pltpu.VMEM((length, width), dtype)
    any_spec = pl.BlockSpec(memory_space=pl.ANY)
    dma = lambda *shape: pltpu.SemaphoreType.DMA(shape)
    layer, gq, gk, gv = pl.pallas_call(
        functools.partial(kernel, n_seq, heads, length, half_d),
        out_shape=(
            jax.ShapeDtypeStruct(grad_out.shape, BF16),
            jax.ShapeDtypeStruct(query_in.shape, BF16),
            jax.ShapeDtypeStruct(query_in.shape, BF16),
            jax.ShapeDtypeStruct(query_in.shape, BF16),
        ),
        in_specs=[pl.BlockSpec(memory_space=pltpu.HBM)] * 6,
        out_specs=(any_spec,) * 4,
        scratch_shapes=[
            wide(BF16), wide(BF16), wide(BF16),
            pltpu.VMEM((HD, length), jnp.int32),
            pltpu.VMEM((length, HD), F32),
            pltpu.VMEM(out_weight.shape, BF16),
            pltpu.VMEM((length, half_d), BF16),
            pltpu.VMEM((length, half_d), BF16),
            pltpu.VMEM((width, half_d), BF16),
            pltpu.VMEM((3, half, half), F32),
            pltpu.VMEM((span, length, HD), BF16),
            wide(F32), wide(BF16),
            pltpu.VMEM((heads, HD, HD), F32),
            pltpu.VMEM((span, heads, HD, HD), BF16),
            pltpu.VMEM((heads, HD, HD), BF16),
            pltpu.VMEM((span, heads, HD, HD), F32),
            pltpu.VMEM((span, heads, HD, HD), BF16),
            pltpu.VMEM((span, 4, heads, HD, HD), BF16),
            pltpu.VMEM((heads, HD, HD), F32),
            wide(F32), wide(F32), wide(F32), wide(F32),
            wide(BF16), wide(BF16),
            pltpu.VMEM((length, half_d), BF16),
            wide(BF16), wide(BF16), wide(BF16),
            pltpu.VMEM((4, heads, HD, HD), BF16),
            pltpu.VMEM((2, heads, HD, length), BF16),
            dma(6), dma(4), dma(2), dma(2), dma(heads), dma(heads),
            dma(span, 2, heads), dma(span, heads), dma(span, heads), dma(span, 4, heads),
            dma(2, heads), dma(4, heads), pltpu.SemaphoreType.REGULAR((4,)),
        ],
        compiler_params=pltpu.CompilerParams(collective_id=0, has_side_effects=True),
        name="log_linear",
    )(query_in, key_in, value_in, jnp.swapaxes(level_mask, 1, 2), out_weight, grad_out)
    results = (layer, gq, gk, gv)
    pieces = [(0, i * length // 4, length // 4) for i in range(4)]
    pieces += [(which, i * half, half) for which in (1, 2, 3) for i in range(2)]
    return pl.pallas_call(
        functools.partial(settle, pieces),
        out_shape=tuple(jax.ShapeDtypeStruct(x.shape, x.dtype) for x in results),
        in_specs=[any_spec] * 4,
        out_specs=(any_spec,) * 4,
        scratch_shapes=[pltpu.VMEM(x.shape[1:], x.dtype) for x in results]
        + [dma(len(pieces)), dma(len(pieces))],
        name="settle",
    )(*results)


def solution(mesh):
    return jax.shard_map(
        on_device,
        mesh=mesh,
        in_specs=(
            P(("groups", "batch"), "seq", "head"),
            P(("groups", "batch"), "seq", "head"),
            P(("groups", "batch"), "seq", "head"),
            P(("groups", "batch"), "seq", None),
            P("head", None),
            P(("groups", "batch"), "seq", "head"),
        ),
        out_specs=(
            P(("groups", "batch"), "seq", "head"),
            P(("groups", "batch"), "seq", "head"),
            P(("groups", "batch"), "seq", "head"),
            P(("groups", "batch"), "seq", "head"),
        ),
        check_vma=False,
    )
```
